16 devices in a mesh: rep: 4 (over z, y), data: 4 (over x, core).
Axes of the slice: x: 2, y: 2, z: 2, core: 2. Of those that a mesh axis runs over, the one named last changes fastest.
Arguments:
- x_now: bfloat16 [32, 256, 1024], P(('rep', 'data'))
- x_next: bfloat16 [32, 256, 1024], P(('rep', 'data'))
- labels: int32 [32], P(('rep', 'data'))
- w_up: float32 [6, 1024, 4096], replicated
- w_down: float32 [6, 4096, 1024], replicated
- w_head: float32 [1024, 1000], replicated
- mom_up: float32 [6, 1024, 4096], replicated
- mom_down: float32 [6, 4096, 1024], replicated
- mom_head: float32 [1024, 1000], replicated
- learn_rate: float32 [], replicated
- momentum: float32 [], replicated
Outputs:
- output 1: float32 [32, 1000], P(('rep', 'data'))
- output 2: float32 [6, 1024, 4096], replicated
- output 3: float32 [6, 4096, 1024], replicated
- output 4: float32 [1024, 1000], replicated
- output 5: float32 [6, 1024, 4096], replicated
- output 6: float32 [6, 4096, 1024], replicated
- output 7: float32 [1024, 1000], replicated
All inputs are finite; a program needn't handle non-finite values.
Results may differ from the reference program's by a relative error of at most 0.0111779.
Values are sent between devices in bfloat16 or wider.
A program may use at most 3.25 GiB of HBM per device.

```python
import jax
import jax.numpy as jnp
from jax import lax

D = 1024
FF = 4096
SEQ = 256
CLASSES = 1000
LAYERS = 6
BATCH_DEV = 2
DEVICES = 16
BATCH = BATCH_DEV * DEVICES
ROWS = BATCH_DEV * SEQ
LN_EPS = 1e-6


def setup_inputs(seed: int = 0) -> dict:
    root_key = jax.random.key(seed)
    subkeys = jax.random.split(root_key, 12)
    mom_scale = 0.5 * BATCH ** -0.5
    x_now = (jax.random.normal(subkeys[0], (BATCH, 1, D), jnp.float32)
             + jax.random.normal(subkeys[1], (BATCH, SEQ, D), jnp.float32)).astype(jnp.bfloat16)
    x_next = (jax.random.normal(subkeys[2], (BATCH, 1, D), jnp.float32)
              + jax.random.normal(subkeys[3], (BATCH, SEQ, D), jnp.float32)).astype(jnp.bfloat16)
    labels = jax.random.randint(subkeys[4], (BATCH,), 0, CLASSES, jnp.int32)
    w_up = jax.random.normal(subkeys[5], (LAYERS, D, FF), jnp.float32) * D ** -0.5
    w_down = jax.random.normal(subkeys[6], (LAYERS, FF, D), jnp.float32) * FF ** -0.5
    w_head = jax.random.normal(subkeys[7], (D, CLASSES), jnp.float32) * D ** -0.5
    mom_up = jax.random.normal(subkeys[8], (LAYERS, D, FF), jnp.float32) * (D ** -0.5 * mom_scale)
    mom_down = jax.random.normal(subkeys[9], (LAYERS, FF, D), jnp.float32) * (FF ** -0.5 * mom_scale)
    mom_head = jax.random.normal(subkeys[10], (D, CLASSES), jnp.float32) * (D ** -0.5 * mom_scale)
    rate_key, coef_key = jax.random.split(subkeys[11])
    learn_rate = jax.random.uniform(rate_key, (), jnp.float32, 0.15, 0.45) * BATCH ** 0.5
    momentum = jax.random.uniform(coef_key, (), jnp.float32, 0.5, 0.95)
    return {'x_now': x_now, 'x_next': x_next, 'labels': labels, 'w_up': w_up, 'w_down': w_down,
            'w_head': w_head, 'mom_up': mom_up, 'mom_down': mom_down, 'mom_head': mom_head,
            'learn_rate': learn_rate, 'momentum': momentum}


def layer_norm(residual):
    centered = residual - jnp.mean(residual, axis=-1, keepdims=True)
    inv_std = lax.rsqrt(jnp.mean(centered * centered, axis=-1, keepdims=True) + LN_EPS)
    return centered * inv_std, inv_std


def norm_back(normed, inv_std, grad_out):
    return inv_std * (grad_out - jnp.mean(grad_out, axis=-1, keepdims=True)
                      - normed * jnp.mean(grad_out * normed, axis=-1, keepdims=True))


def gelu_parts(pre_act):
    gauss_cdf = 0.5 * (1.0 + lax.erf(pre_act * 0.7071067811865476))
    density = jnp.exp(-0.5 * pre_act * pre_act) * 0.3989422804014327
    return pre_act * gauss_cdf, gauss_cdf + pre_act * density


def block_forward(residual, up_bf, down_bf):
    normed, inv_std = layer_norm(residual)
    act_in = normed.astype(jnp.bfloat16)
    pre_act = jnp.dot(act_in, up_bf, preferred_element_type=jnp.float32)
    hidden, gelu_slope = gelu_parts(pre_act)
    hid_bf = hidden.astype(jnp.bfloat16)
    result = residual + jnp.dot(hid_bf, down_bf, preferred_element_type=jnp.float32)
    return result, (normed, inv_std, act_in, gelu_slope, hid_bf)


def pool_logits(residual, head_bf):
    pooled = jnp.mean(residual.reshape(BATCH_DEV, SEQ, D), axis=1).astype(jnp.bfloat16)
    return pooled, jnp.dot(pooled, head_bf, preferred_element_type=jnp.float32)


def shard_grads(x_shard, label_shard, up_bf, down_bf, head_bf):
    residual = x_shard.reshape(ROWS, D).astype(jnp.float32)

    def fwd_layer(resid_in, weights):
        return block_forward(resid_in, weights[0], weights[1])

    final_res, saved_acts = lax.scan(fwd_layer, residual, (up_bf, down_bf))
    pooled, logits = pool_logits(final_res, head_bf)
    soft_probs = jax.nn.softmax(logits, axis=-1)
    onehot = (label_shard[:, None] == jnp.arange(CLASSES, dtype=jnp.int32)[None, :]).astype(jnp.float32)
    d_logits = ((soft_probs - onehot) / BATCH).astype(jnp.bfloat16)
    grad_head = jnp.dot(pooled.T, d_logits, preferred_element_type=jnp.float32)
    d_pooled = jnp.dot(d_logits, head_bf.T, preferred_element_type=jnp.float32)
    d_resid = jnp.broadcast_to((d_pooled / SEQ)[:, None, :], (BATCH_DEV, SEQ, D)).reshape(ROWS, D)

    def back_layer(d_carry, layer_data):
        up_w, down_w, normed, inv_std, act_in, gelu_slope, hid_bf = layer_data
        d_out = d_carry.astype(jnp.bfloat16)
        grad_down = jnp.dot(hid_bf.T, d_out, preferred_element_type=jnp.float32)
        d_hidden = jnp.dot(d_out, down_w.T, preferred_element_type=jnp.float32)
        d_pre = (d_hidden * gelu_slope).astype(jnp.bfloat16)
        grad_up = jnp.dot(act_in.T, d_pre, preferred_element_type=jnp.float32)
        d_normed = jnp.dot(d_pre, up_w.T, preferred_element_type=jnp.float32)
        d_new = d_carry + norm_back(normed, inv_std, d_normed)
        return d_new, (grad_up.astype(jnp.bfloat16), grad_down.astype(jnp.bfloat16))

    _, (grad_up, grad_down) = lax.scan(back_layer, d_resid, (up_bf, down_bf) + saved_acts, reverse=True)
    return grad_up, grad_down, grad_head.astype(jnp.bfloat16)


def reference(x_now, x_next, labels, w_up, w_down, w_head, mom_up, mom_down, mom_head, learn_rate, momentum):
    up_bf = w_up.astype(jnp.bfloat16)
    down_bf = w_down.astype(jnp.bfloat16)
    head_bf = w_head.astype(jnp.bfloat16)

    def accumulate(grad_sums, shard_data):
        grad_parts = shard_grads(shard_data[0], shard_data[1], up_bf, down_bf, head_bf)
        new_sums = tuple(grad_sum + grad_part.astype(jnp.float32) for grad_sum, grad_part in zip(grad_sums, grad_parts))
        return new_sums, None

    zero_init = (jnp.zeros_like(w_up), jnp.zeros_like(w_down), jnp.zeros_like(w_head))
    shard_inputs = (x_now.reshape(DEVICES, BATCH_DEV, SEQ, D), labels.reshape(DEVICES, BATCH_DEV))
    (sum_up, sum_down, sum_head), _ = lax.scan(accumulate, zero_init, shard_inputs)
    new_mom_up = momentum * mom_up + sum_up
    new_mom_down = momentum * mom_down + sum_down
    new_mom_head = momentum * mom_head + sum_head
    new_up = w_up - learn_rate * new_mom_up
    new_down = w_down - learn_rate * new_mom_down
    new_head = w_head - learn_rate * new_mom_head
    next_up = new_up.astype(jnp.bfloat16)
    next_down = new_down.astype(jnp.bfloat16)
    next_head = new_head.astype(jnp.bfloat16)

    def shard_logits(x_shard):
        residual = x_shard.reshape(ROWS, D).astype(jnp.float32)

        def fwd_layer(resid_in, weights):
            return block_forward(resid_in, weights[0], weights[1])[0], None

        final_res, _ = lax.scan(fwd_layer, residual, (next_up, next_down))
        return pool_logits(final_res, next_head)[1]

    logits_next = lax.map(shard_logits, x_next.reshape(DEVICES, BATCH_DEV, SEQ, D)).reshape(BATCH, CLASSES)
    return (logits_next, new_up, new_down, new_head, new_mom_up, new_mom_down, new_mom_head)
```

```python
import functools

import jax
import jax.numpy as jnp
from jax import lax
from jax.experimental import pallas as pl
from jax.experimental.pallas import tpu as pltpu
from jax.sharding import PartitionSpec as P


LN_EPS = 1e-6
BATCH_AXES = ('rep', 'data')
BLOCKS = 16
BW = 256
LINKS = (2, 4, 8)
ADMIT = ((5, 1), (5, 0), (4, 1), (4, 0)) + tuple((l, k) for l in range(4) for k in (0, 1))
GATHER_SC = frozenset(m for i, m in enumerate(ADMIT) if i % 2 == 0)

ORDER = tuple((t[0], int(t[1]), int(t[2])) for t in (
    'g51', 'S50', 'a51', 'g50', 'N50', 'g41', 'a50', 'S40', 'a41', 'g40',
    'N40', 'b51', 'a40', 'S30', 'b50', 'N30', 'S20', 'c51', 'b41', 'N20',
    'c50', 'b40', 'g11', 'S10', 'd51', 'c41', 'g10', 'N10', 'd50', 'c40',
    'g01', 'S00', 'a01', 'a10', 'd40', 'a11', 'd41', 'e50', 'g00', 'g20',
    'g21', 'g30', 'U51', 'e40', 'b01', 'b10', 'b11', 'U41', 'H00', 'g31',
    'a00', 'c01', 'a20', 'f50', 'f40', 'c11', 'c10', 'a21', 'h40', 'b20',
    'b00', 'd11', 'U40', 'd01', 'd10', 'c00', 'b21', 'h50', 'U50', 'e01',
    'e11', 'c20', 'a30', 'a31', 'f11', 'c21', 'd00', 'd20', 'f01', 'b31',
    'd21', 'b30', 'K00', 'h11', 'c31', 'h01', 'K01', 'd31', 'e21', 'c30',
    'K10', 'd30', 'e31', 'K11', 'f21', 'K20', 'f31', 'h21', 'h31', 'K21',
    'K30', 'K31', 'F40', 'F41', 'F50', 'F51',
))


def layer_norm(residual):
    centered = residual - jnp.mean(residual, axis=-1, keepdims=True)
    inv_std = lax.rsqrt(jnp.mean(centered * centered, axis=-1, keepdims=True) + LN_EPS)
    return centered * inv_std, inv_std


def norm_back(normed, inv_std, grad_out):
    return inv_std * (grad_out - jnp.mean(grad_out, axis=-1, keepdims=True)
                      - normed * jnp.mean(grad_out * normed, axis=-1, keepdims=True))


def gelu(pre_act):
    return pre_act * (0.5 * (1.0 + lax.erf(pre_act * 0.7071067811865476)))


def gelu_parts(pre_act):
    gauss_cdf = 0.5 * (1.0 + lax.erf(pre_act * 0.7071067811865476))
    density = jnp.exp(-0.5 * pre_act * pre_act) * 0.3989422804014327
    return pre_act * gauss_cdf, gauss_cdf + pre_act * density


def pool_logits(residual, images, head_bf):
    pooled = jnp.mean(residual.reshape(images, -1, residual.shape[-1]), axis=1).astype(jnp.bfloat16)
    return pooled, jnp.dot(pooled, head_bf, preferred_element_type=jnp.float32)


def order_of(m):
    i = ADMIT.index(m) % 3
    return tuple(LINKS[(i + s) % 3] for s in range(3))


def flip(a, b):
    out = 0
    for s in range(4):
        x = lax.rem(lax.div(a, 1 << s), 2)
        y = lax.rem(lax.div(b, 1 << s), 2)
        out = out + (x + y - 2 * x * y) * (1 << s)
    return out


def block_at(pos, order, me):
    vals = (1,) + order
    mask = 0
    for s in range(4):
        mask = mask + lax.rem(lax.div(pos, 1 << (3 - s)), 2) * vals[s]
    return flip(mask, me)


def dot_tn(a, b):
    return lax.dot_general(a, b, (((0,), (0,)), ((), ())), preferred_element_type=jnp.float32)


def grad_down_send(me_ref, z_ref, v_ref, o_ref):
    o_ref[...] = dot_tn(z_ref[...], v_ref[...]).astype(jnp.bfloat16)


def grad_up_send(me_ref, a_ref, s_ref, o_ref, at_ref):
    @pl.when(pl.program_id(0) == 0)
    def _():
        at_ref[...] = a_ref[...].astype(jnp.float32).T.astype(jnp.bfloat16)

    o_ref[...] = jnp.dot(at_ref[...], s_ref[...], preferred_element_type=jnp.float32).astype(jnp.bfloat16)


def grad_down_keep(me_ref, z_ref, v_ref, r_ref, os_ref, ok_ref):
    g = dot_tn(z_ref[...], v_ref[...]).astype(jnp.bfloat16)
    out = (g.astype(jnp.float32) + r_ref[...].astype(jnp.float32)).astype(jnp.bfloat16)

    @pl.when(pl.program_id(0) < 4)
    def _():
        os_ref[...] = out

    @pl.when(pl.program_id(0) >= 4)
    def _():
        ok_ref[...] = out


def grad_up_keep(me_ref, a_ref, s_ref, r_ref, os_ref, ok_ref, at_ref):
    @pl.when(pl.program_id(0) == 0)
    def _():
        at_ref[...] = a_ref[...].astype(jnp.float32).T.astype(jnp.bfloat16)

    g = jnp.dot(at_ref[...], s_ref[...], preferred_element_type=jnp.float32).astype(jnp.bfloat16)
    out = (g.astype(jnp.float32) + r_ref[...].astype(jnp.float32)).astype(jnp.bfloat16)

    @pl.when(pl.program_id(0) < 4)
    def _():
        os_ref[...] = out

    @pl.when(pl.program_id(0) >= 4)
    def _():
        ok_ref[...] = out


def grad_send(m, me, left, right):
    order = order_of(m)
    rows, dim = left.shape[0], 1024
    if m[1] == 1:
        return pl.pallas_call(
            grad_down_send,
            grid_spec=pltpu.PrefetchScalarGridSpec(
                num_scalar_prefetch=1, grid=(8,),
                in_specs=[pl.BlockSpec((rows, BW), lambda i, me: (0, block_at(i + 8, order, me[0]))),
                          pl.BlockSpec((rows, dim), lambda i, me: (0, 0))],
                out_specs=pl.BlockSpec((BW, dim), lambda i, me: (i, 0))),
            out_shape=jax.ShapeDtypeStruct((8 * BW, dim), jnp.bfloat16),
            cost_estimate=pl.CostEstimate(flops=2 * rows * dim * 8 * BW, bytes_accessed=7 << 20, transcendentals=0),
            name='gds')(me, left, right)
    return pl.pallas_call(
        grad_up_send,
        grid_spec=pltpu.PrefetchScalarGridSpec(
            num_scalar_prefetch=1, grid=(8,),
            in_specs=[pl.BlockSpec((rows, dim), lambda i, me: (0, 0)),
                      pl.BlockSpec((rows, BW), lambda i, me: (0, block_at(i + 8, order, me[0])))],
            out_specs=pl.BlockSpec((dim, BW), lambda i, me: (0, i)),
            scratch_shapes=[pltpu.VMEM((dim, rows), jnp.bfloat16)]),
        out_shape=jax.ShapeDtypeStruct((dim, 8 * BW), jnp.bfloat16),
        cost_estimate=pl.CostEstimate(flops=2 * rows * dim * 8 * BW, bytes_accessed=7 << 20, transcendentals=0),
        name='gus')(me, left, right)


def grad_keep(m, me, left, right, got):
    order = order_of(m)
    rows, dim = left.shape[0], 1024
    spot = lambda i: lax.rem(i + 4, 8)
    low = lambda i: jnp.minimum(i, 3)
    high = lambda i: jnp.maximum(i - 4, 0)
    if m[1] == 1:
        return pl.pallas_call(
            grad_down_keep,
            grid_spec=pltpu.PrefetchScalarGridSpec(
                num_scalar_prefetch=1, grid=(8,),
                in_specs=[pl.BlockSpec((rows, BW), lambda i, me: (0, block_at(spot(i), order, me[0]))),
                          pl.BlockSpec((rows, dim), lambda i, me: (0, 0)),
                          pl.BlockSpec((BW, dim), lambda i, me: (spot(i), 0))],
                out_specs=[pl.BlockSpec((BW, dim), lambda i, me: (low(i), 0)),
                           pl.BlockSpec((BW, dim), lambda i, me: (high(i), 0))]),
            out_shape=[jax.ShapeDtypeStruct((4 * BW, dim), jnp.bfloat16)] * 2,
            cost_estimate=pl.CostEstimate(flops=2 * rows * dim * 8 * BW, bytes_accessed=11 << 20, transcendentals=0),
            name='gdk')(me, left, right, got)
    return pl.pallas_call(
        grad_up_keep,
        grid_spec=pltpu.PrefetchScalarGridSpec(
            num_scalar_prefetch=1, grid=(8,),
            in_specs=[pl.BlockSpec((rows, dim), lambda i, me: (0, 0)),
                      pl.BlockSpec((rows, BW), lambda i, me: (0, block_at(spot(i), order, me[0]))),
                      pl.BlockSpec((dim, BW), lambda i, me: (0, spot(i)))],
            out_specs=[pl.BlockSpec((dim, BW), lambda i, me: (0, low(i))),
                       pl.BlockSpec((dim, BW), lambda i, me: (0, high(i)))],
            scratch_shapes=[pltpu.VMEM((dim, rows), jnp.bfloat16)]),
        out_shape=[jax.ShapeDtypeStruct((dim, 4 * BW), jnp.bfloat16)] * 2,
        cost_estimate=pl.CostEstimate(flops=2 * rows * dim * 8 * BW, bytes_accessed=11 << 20, transcendentals=0),
        name='guk')(me, left, right, got)


def update_body(kind, pieces, *refs):
    _, rates_ref = refs[:2]
    refs = refs[2:]
    acts = ()
    if kind == 'up':
        acts, refs = refs[:1], refs[1:]
    elif kind == 'down':
        acts, refs = refs[:2], refs[2:]
    grads, refs = refs[:pieces], refs[pieces:]
    w_ref, m_ref = refs[:2]
    nw_ref, nm_ref = refs[-2 - {'up': 2, 'down': 1, 'plain': 1}[kind]:][:2]
    outs = refs[-{'up': 2, 'down': 1, 'plain': 1}[kind]:]
    step = pl.program_id(0)

    if kind == 'up':
        @pl.when(step == 0)
        def _():
            outs[1][...] = layer_norm(acts[0][...])[0].astype(jnp.bfloat16)
    if kind == 'down':
        @pl.when(step == 0)
        def _():
            outs[0][...] = acts[0][...]

    def apply(grad_ref):
        grad = grad_ref[...]
        shape = w_ref.shape[1:]
        new_m = rates_ref[1] * m_ref[...].reshape(shape) + grad.reshape(shape).astype(jnp.float32)
        new_w = w_ref[...].reshape(shape) - rates_ref[0] * new_m
        nm_ref[...] = new_m.reshape(nm_ref.shape)
        nw_ref[...] = new_w.reshape(nw_ref.shape)
        new_bf = new_w.astype(jnp.bfloat16)
        if kind == 'up':
            outs[0][...] = gelu(jnp.dot(outs[1][...], new_bf, preferred_element_type=jnp.float32)).astype(jnp.bfloat16)
        elif kind == 'down':
            outs[0][...] += jnp.dot(acts[1][...], new_bf, preferred_element_type=jnp.float32)
        else:
            outs[0][...] = new_bf

    if pieces == 1:
        apply(grads[0])
    else:
        for p in range(pieces):
            pl.when(lax.div(step, 4) == p)(functools.partial(apply, grads[p]))


def update(m, kind, me, rates, acts, grads, w, mom, into):
    l, k = m
    order = order_of(m)
    sc = len(grads) == 1
    dim, hid, rows = 1024, 4096, 512
    natural = (lambda i, me: i) if sc else (lambda i, me: block_at(i, order, me[0]))
    part = lambda p, i: jnp.clip(i - 4 * p, 0, 3)
    if k == 0:
        w_spec = pl.BlockSpec((1, dim, BW), lambda i, me: (l, 0, natural(i, me)))
        bf_spec, bf_shape = pl.BlockSpec((dim, BW), lambda i, me: (0, natural(i, me))), (dim, hid)
        if sc:
            g_specs = [pl.BlockSpec((1, dim, BW), lambda i, me: (i, 0, 0))]
        else:
            g_specs = [pl.BlockSpec((dim, BW), lambda i, me, p=p: (0, part(p, i))) for p in range(4)]
    else:
        w_spec = pl.BlockSpec((1, BW, dim), lambda i, me: (l, natural(i, me), 0))
        bf_spec, bf_shape = pl.BlockSpec((BW, dim), lambda i, me: (natural(i, me), 0)), (hid, dim)
        if sc:
            g_specs = [pl.BlockSpec((1, BW, dim), lambda i, me: (i, 0, 0))]
        else:
            g_specs = [pl.BlockSpec((BW, dim), lambda i, me, p=p: (part(p, i), 0)) for p in range(4)]
    whole = pl.BlockSpec((rows, dim), lambda i, me: (0, 0))
    z_spec = pl.BlockSpec((rows, BW), lambda i, me: (0, natural(i, me)))
    scratch = []
    if kind == 'up':
        act_specs = [whole]
        last, last_shape = z_spec, jax.ShapeDtypeStruct((rows, hid), jnp.bfloat16)
        scratch = [pltpu.VMEM((rows, dim), jnp.bfloat16)]
    elif kind == 'down':
        act_specs = [whole, z_spec]
        last, last_shape = whole, jax.ShapeDtypeStruct((rows, dim), jnp.float32)
    else:
        act_specs = []
        last, last_shape = bf_spec, jax.ShapeDtypeStruct(bf_shape, jnp.bfloat16)
    any_spec = pl.BlockSpec(memory_space=pl.ANY)
    in_specs = [pl.BlockSpec(memory_space=pltpu.SMEM)] + act_specs + g_specs + [w_spec, w_spec]
    args = [me, rates, *acts, *grads, w, mom]
    aliases = {}
    if into is not None:
        aliases = {len(args): 0, len(args) + 1: 1}
        in_specs += [any_spec, any_spec]
        args += list(into)
    full = jax.ShapeDtypeStruct(w.shape, jnp.float32)
    return pl.pallas_call(
        functools.partial(update_body, kind, len(grads)),
        grid_spec=pltpu.PrefetchScalarGridSpec(
            num_scalar_prefetch=1, grid=(BLOCKS,), in_specs=in_specs,
            out_specs=[w_spec, w_spec, last], scratch_shapes=scratch),
        out_shape=[full, full, last_shape],
        input_output_aliases=aliases,
        compiler_params=pltpu.CompilerParams(vmem_limit_bytes=48 << 20),
        cost_estimate=pl.CostEstimate(flops=10_000_000_000, bytes_accessed=80 << 20, transcendentals=0))(*args)


def solution(mesh):
    num_dev = mesh.shape['rep'] * mesh.shape['data']
    pairs = {bit: [(i, i ^ bit) for i in range(num_dev)] for bit in (1, 2, 4, 8)}

    def local_step(x_now, x_next, labels, w_up, w_down, w_head, mom_up, mom_down, mom_head, learn_rate, momentum):
        images, seq_len, model_dim = x_now.shape
        layers = w_up.shape[0]
        classes = w_head.shape[1]
        rows = images * seq_len
        global_batch = images * num_dev
        weights = (w_up, w_down)
        moms = (mom_up, mom_down)
        me = (lax.axis_index('rep') * mesh.shape['data'] + lax.axis_index('data')).astype(jnp.int32).reshape(1)
        rates = jnp.stack([learn_rate, momentum])
        token = [None]

        def hold(*args):
            if token[0] is None:
                return args
            return lax.optimization_barrier((*args, token[0]))[:-1]

        def cp(x, bit):
            return lax.ppermute(x, BATCH_AXES, pairs[bit])

        residual = x_now.reshape(rows, model_dim).astype(jnp.float32)
        saved = []
        for l in range(layers):
            residual, wu, wd = lax.optimization_barrier((residual, w_up, w_down))
            normed, inv_std = layer_norm(residual)
            act_in = normed.astype(jnp.bfloat16)
            pre_act = jnp.dot(act_in, wu[l].astype(jnp.bfloat16), preferred_element_type=jnp.float32)
            hidden, slope = gelu_parts(pre_act)
            hid_bf = hidden.astype(jnp.bfloat16)
            saved.append((normed, inv_std, act_in, slope, hid_bf))
            residual = residual + jnp.dot(hid_bf, wd[l].astype(jnp.bfloat16), preferred_element_type=jnp.float32)
        head_bf = w_head.astype(jnp.bfloat16)
        pooled, logits = pool_logits(residual, images, head_bf)
        soft_probs = jax.nn.softmax(logits, axis=-1)
        onehot = (labels[:, None] == jnp.arange(classes, dtype=jnp.int32)[None, :]).astype(jnp.float32)
        d_logits = ((soft_probs - onehot) / global_batch).astype(jnp.bfloat16)
        grad_head = jnp.einsum('bd,bc->dc', pooled, d_logits, preferred_element_type=jnp.float32)
        red_head = lax.psum(grad_head.astype(jnp.bfloat16), BATCH_AXES)
        d_pooled = jnp.einsum('bc,dc->bd', d_logits, head_bf, preferred_element_type=jnp.float32)
        d_resid = jnp.broadcast_to((d_pooled / seq_len)[:, None, :], (images, seq_len, model_dim)).reshape(rows, model_dim)

        d_res = {layers - 1: d_resid}
        v_bf = {layers - 1: d_resid.astype(jnp.bfloat16)}
        s_bf = {}
        box = {}
        new = [None, None]
        res_next = {(0, 0): x_next.reshape(rows, model_dim).astype(jnp.float32)}
        z_next = {}
        w_bf = {}

        def cut(x, k, lo, hi):
            n = x.shape[k == 0 and 1 or 0]
            lo, hi = lo * n // 4, hi * n // 4
            return x[:, lo:hi] if k == 0 else x[lo:hi]

        def fadd(a, b):
            return (a.astype(jnp.float32) + b.astype(jnp.float32)).astype(jnp.bfloat16)

        def step(op, l, k):
            m = (l, k)
            if op == 'S':
                normed, inv_std, act_in, slope, hid_bf = saved[l]
                v, sl, w, = hold(v_bf[l], slope, w_down)
                d_hidden = jnp.einsum('td,fd->tf', v, w[l].astype(jnp.bfloat16), preferred_element_type=jnp.float32)
                s_bf[l] = (d_hidden * sl).astype(jnp.bfloat16)
                token[0] = s_bf[l]
                return
            if op == 'N':
                normed, inv_std, act_in, slope, hid_bf = saved[l]
                s, dr, w = hold(s_bf[l], d_res[l], w_up)
                d_normed = jnp.einsum('tf,df->td', s, w[l].astype(jnp.bfloat16), preferred_element_type=jnp.float32)
                d_res[l - 1] = dr + norm_back(normed, inv_std, d_normed)
                v_bf[l - 1] = d_res[l - 1].astype(jnp.bfloat16)
                token[0] = v_bf[l - 1]
                return
            order = order_of(m)
            if op in 'ga':
                left, right = (saved[l][4], v_bf[l]) if k == 1 else (saved[l][2], s_bf[l])
            if op == 'g':
                left, right = hold(left, right)
                out = grad_send(m, me, left, right)
                box['r0', m] = cp(out, 1)
            elif op == 'a':
                left, right, got = hold(left, right, box.pop(('r0', m)))
                out, keep = grad_keep(m, me, left, right, got)
                box['k1', m] = keep
                box['r1', m] = cp(out, order[0])
            elif op in 'bc':
                src, dst = {'b': ('1', '2'), 'c': ('2', '3')}[op]
                keep, got = hold(box.pop(('k' + src, m)), box.pop(('r' + src, m)))
                out = fadd(cut(keep, k, 2, 4), cut(got, k, 2, 4))
                box['k' + dst, m] = fadd(cut(keep, k, 0, 2), cut(got, k, 0, 2))
                box['r' + dst, m] = cp(out, order[1] if op == 'b' else order[2])
                out = box['k' + dst, m]
            elif op == 'd':
                keep, got = hold(box.pop(('k3', m)), box.pop(('r3', m)))
                out = fadd(keep, got)
                if m in GATHER_SC:
                    box['g', m] = (lax.all_gather(out, BATCH_AXES),)
                else:
                    box['p0', m] = out
                    box['q0', m] = cp(out, order[2])
            elif op in 'ef':
                src, dst = {'e': ('0', '1'), 'f': ('1', '2')}[op]
                own, got = hold(box.pop(('p' + src, m)), box.pop(('q' + src, m)))
                out = jnp.concatenate([own, got], axis=1 - k)
                if op == 'e':
                    box['p1', m] = out
                    box['q1', m] = cp(out, order[1])
                else:
                    far = cp(out, order[0])
                    box['g', m] = (out, far, cp(out, 1))
            elif op == 'h':
                own, far, other = box['g', m]
                send, = hold(far)
                box['g', m] = (own, far, other, cp(send, 1))
                return
            elif op in 'KU':
                kind = 'plain' if op == 'U' else ('up' if k == 0 else 'down')
                acts = ()
                if kind == 'up':
                    acts = (res_next[l, 0],)
                elif kind == 'down':
                    acts = (res_next[l, 0], z_next[l])
                held = hold(*acts, *box.pop(('g', m)))
                acts, grads = held[:len(acts)], held[len(acts):]
                nw, nm, out = update(m, kind, me, rates, acts, grads, weights[k], moms[k], new[k])
                new[k] = (nw, nm)
                if kind == 'up':
                    z_next[l] = out
                elif kind == 'down':
                    res_next[l + 1, 0] = out
                else:
                    w_bf[m] = out
            elif op == 'F':
                if k == 0:
                    r, w = hold(res_next[l, 0], w_bf[m])
                    out = gelu(jnp.dot(layer_norm(r)[0].astype(jnp.bfloat16), w,
                                       preferred_element_type=jnp.float32)).astype(jnp.bfloat16)
                    z_next[l] = out
                else:
                    r, z, w = hold(res_next[l, 0], z_next[l], w_bf[m])
                    out = r + jnp.dot(z, w, preferred_element_type=jnp.float32)
                    res_next[l + 1, 0] = out
            elif op == 'H':
                red, mh, wh = hold(red_head, mom_head, w_head)
                nm = momentum * mh + red.astype(jnp.float32)
                nw = wh - learn_rate * nm
                box['head'] = (nw, nm)
                out = nm
            token[0] = out

        for op, l, k in ORDER:
            step(op, l, k)
        new_head, new_mom_head = box['head']
        _, logits_next = pool_logits(res_next[layers, 0], images, new_head.astype(jnp.bfloat16))
        return logits_next, new[0][0], new[1][0], new_head, new[0][1], new[1][1], new_mom_head

    batch_spec = P(BATCH_AXES)
    whole_spec = P()
    return jax.shard_map(local_step, mesh=mesh,
                         in_specs=(batch_spec, batch_spec, batch_spec) + (whole_spec,) * 8,
                         out_specs=(batch_spec,) + (whole_spec,) * 6,
                         check_vma=False)
```

```python
import functools

import jax
import jax.numpy as jnp
from jax import lax
from jax.experimental import pallas as pl
from jax.experimental.pallas import tpu as pltpu
from jax.sharding import PartitionSpec as P


LN_EPS = 1e-6
BATCH_AXES = ('rep', 'data')
NB = 8
HB = 512
NS = 4
LINKS = (1, 2, 4)
ADMIT = ((5, 1), (5, 0), (4, 1), (0, 0), (0, 1), (1, 0), (1, 1), (2, 0), (2, 1), (3, 0), (3, 1), (4, 0),)
GATHER_SC = ((0, 0), (4, 1), (5, 0), (5, 1),)
ORDER = tuple((t[0], int(t[1]), int(t[2])) for t in (
    'B50', 'a51', 'a50', 'B40', 'a41', 'B30', 'b51', 'b50', 'B20', 'c51', 'b41', 'B10',
    'd51', 'c50', 'c41', 'B00', 'a00', 'a01', 'a10', 'a11', 'a20', 'a21', 'd50', 'd41',
    'H00', 'U51', 'b00', 'b01', 'b10', 'b11', 'b20', 'b21', 'U50', 'a30', 'a31', 'a40',
    'c10', 'c00', 'c01', 'U41', 'c11', 'c20', 'c21', 'b30', 'b31', 'b40', 'd01', 'd00',
    'd10', 'd20', 'd11', 'd21', 'c40', 'c30', 'c31', 'e01', 'e10', 'e11', 'K00', 'd30',
    'd31', 'd40', 'e20', 'e21', 'f01', 'e30', 'f10', 'e31', 'e40', 'f11', 'f20', 'f21',
    'f40', 'h01', 'K01', 'h10', 'f30', 'f31', 'h11', 'K10', 'h20', 'K11', 'h21', 'h30',
    'K20', 'h31', 'K21', 'h40', 'K30', 'K31', 'K40', 'F41', 'F50', 'F51',
))


def layer_norm(residual):
    centered = residual - jnp.mean(residual, axis=-1, keepdims=True)
    inv_std = lax.rsqrt(jnp.mean(centered * centered, axis=-1, keepdims=True) + LN_EPS)
    return centered * inv_std, inv_std


def norm_back(normed, inv_std, grad_out):
    return inv_std * (grad_out - jnp.mean(grad_out, axis=-1, keepdims=True)
                      - normed * jnp.mean(grad_out * normed, axis=-1, keepdims=True))


def gelu(pre_act):
    return pre_act * (0.5 * (1.0 + lax.erf(pre_act * 0.7071067811865476)))


def gelu_parts(pre_act):
    gauss_cdf = 0.5 * (1.0 + lax.erf(pre_act * 0.7071067811865476))
    density = jnp.exp(-0.5 * pre_act * pre_act) * 0.3989422804014327
    return pre_act * gauss_cdf, gauss_cdf + pre_act * density


def pool_logits(residual, images, head_bf):
    pooled = jnp.mean(residual.reshape(images, -1, residual.shape[-1]), axis=1).astype(jnp.bfloat16)
    return pooled, jnp.dot(pooled, head_bf, preferred_element_type=jnp.float32)


def order_of(m):
    i = ADMIT.index(m) % 3
    return tuple(LINKS[(i + s) % 3] for s in range(3))


def unmask(block, order):
    return ((block // order[0]) % 2) * 4 + ((block // order[1]) % 2) * 2 + (block // order[2]) % 2


def flip(a, b):
    out = 0
    for v in (1, 2, 4):
        x, y = (a // v) % 2, (b // v) % 2
        out = out + (x + y - 2 * x * y) * v
    return out


def place():
    rep, data = lax.axis_index('rep'), lax.axis_index('data')
    return rep, data, rep * 2 + data // 2, data % 2


def dot(a, b, ca=1, cb=0):
    return lax.dot_general(a, b, (((ca,), (cb,)), ((), ())), preferred_element_type=jnp.float32)


def add_bf(a, b):
    return (a.astype(jnp.float32) + b.astype(jnp.float32)).astype(jnp.bfloat16)


ANY = pl.BlockSpec(memory_space=pl.ANY)
WHOLE = pl.BlockSpec(memory_space=pltpu.VMEM)
DMA = pltpu.SemaphoreType.DMA
F32, BF16 = jnp.float32, jnp.bfloat16


def back_body(l, last, order_up, order_down, v_ref, d_ref, r_ref, w1_ref, w2_ref, slope_ref, z_ref, *refs):
    up_s, up_k, down_s, down_k = refs[:4]
    refs = refs[4:]
    if not last:
        dn_ref, vn_ref = refs[:2]
        refs = refs[2:]
    (w1, w2, sl, zb, at_own, at_far, v_own, v_far, mine, far, got, acc,
     in_sem, out_sem, send_sem, recv_sem) = refs
    rep, data, chip, core = place()
    peer = (rep, data + 1 - 2 * core)
    barrier = pltpu.get_barrier_semaphore()

    def load(i, slot):
        cols = pl.ds(pl.multiple_of(i * HB, HB), HB)
        return (pltpu.make_async_copy(w2_ref.at[l, cols, :], w2.at[slot], in_sem.at[0, slot]),
                pltpu.make_async_copy(slope_ref.at[:, cols], sl.at[slot], in_sem.at[1, slot]),
                pltpu.make_async_copy(z_ref.at[:, cols], zb.at[slot], in_sem.at[2, slot]),
                pltpu.make_async_copy(w1_ref.at[l, :, cols], w1.at[slot], in_sem.at[3, slot]))

    def start(i, slot):
        for copy in load(i, slot):
            copy.start()

    def remote(i, k):
        return pltpu.make_async_remote_copy(
            src_ref=far.at[i % NS, k], dst_ref=got.at[i % NS, k],
            send_sem=send_sem.at[i % NS, k], recv_sem=recv_sem.at[i % NS, k],
            device_id=peer, device_id_type=pl.DeviceIdType.MESH)

    def stores(i):
        block = flip(i, chip)
        out = []
        for k, (os, ok, order) in enumerate(((up_s, up_k, order_up), (down_s, down_k, order_down))):
            pos = unmask(block, order)
            out.append((pos // 4, pltpu.make_async_copy(mine.at[i % NS, k], os.at[pos % 4], out_sem.at[i % NS, k]),
                        pltpu.make_async_copy(mine.at[i % NS, k], ok.at[pos % 4], out_sem.at[i % NS, k])))
        return out

    def finish(i):
        for k in (0, 1):
            remote(i, k).wait_recv()
            mine[i % NS, k] = add_bf(mine[i % NS, k], got[i % NS, k])
        for high, to_send, to_keep in stores(i):
            @pl.when(high == 1)
            def _():
                to_send.start()

            @pl.when(high == 0)
            def _():
                to_keep.start()

    def settle(i):
        for k in (0, 1):
            remote(i, k).wait_send()
        for high, to_send, to_keep in stores(i):
            @pl.when(high == 1)
            def _():
                to_send.wait()

            @pl.when(high == 0)
            def _():
                to_keep.wait()

    start(0, 0)
    start(1, 1)
    pl.semaphore_signal(barrier, inc=1, device_id=peer, device_id_type=pl.DeviceIdType.MESH)
    residual = r_ref[...]
    normed, inv_std = layer_norm(residual)
    a_t = normed.astype(BF16).T
    own, other = pl.ds(pl.multiple_of(core * HB, HB), HB), pl.ds(pl.multiple_of((1 - core) * HB, HB), HB)
    acc[...] = jnp.zeros_like(acc)
    at_own[...] = a_t[:HB]
    at_far[...] = a_t[HB:]
    v_own[...] = v_ref[:, own]
    v_far[...] = v_ref[:, other]

    @pl.when(core == 1)
    def _():
        tmp = at_own[...]
        at_own[...] = at_far[...]
        at_far[...] = tmp

    pl.semaphore_wait(barrier, 1)

    def step(i, _):
        slot = i % 3

        @pl.when(i + 2 < NB)
        def _():
            start(i + 2, (i + 2) % 3)

        @pl.when(i >= NS)
        def _():
            settle(i - NS)

        copies = load(i, slot)
        copies[0].wait()
        copies[1].wait()
        s = (dot(v_ref[...], w2[slot].astype(BF16), 1, 1) * sl[slot]).astype(BF16)
        far[i % NS, 0] = dot(at_far[...], s).astype(BF16)
        remote(i, 0).start()
        copies[2].wait()
        z_t = zb[slot].T
        far[i % NS, 1] = dot(z_t, v_far[...]).astype(BF16)
        remote(i, 1).start()
        mine[i % NS, 0] = dot(at_own[...], s).astype(BF16)
        mine[i % NS, 1] = dot(z_t, v_own[...]).astype(BF16)
        copies[3].wait()
        if not last:
            acc[...] += dot(s, w1[slot].astype(BF16), 1, 1)

        @pl.when(i > 0)
        def _():
            finish(i - 1)

        return 0

    lax.fori_loop(0, NB, step, 0)
    finish(NB - 1)
    if not last:
        residual = r_ref[...]
        normed, inv_std = layer_norm(residual)
        grad = d_ref[...] + norm_back(normed, inv_std, acc[...])
        dn_ref[...] = grad
        vn_ref[...] = grad.astype(BF16)

    for i in range(NB - NS, NB):
        settle(i)


def back(l, v, d, r, w_up, w_down, slope, z):
    rows, dim, hid = 512, 1024, 4096
    last = l == 0
    tile = jax.ShapeDtypeStruct((4, HB, HB), BF16)
    outs, specs = [tile] * 4, [ANY] * 4
    if not last:
        outs += [jax.ShapeDtypeStruct((rows, dim), F32), jax.ShapeDtypeStruct((rows, dim), BF16)]
        specs += [WHOLE, WHOLE]
    return pl.pallas_call(
        functools.partial(back_body, l, last, order_of((l, 0)), order_of((l, 1))),
        out_shape=outs, in_specs=[WHOLE, WHOLE, WHOLE, ANY, ANY, ANY, ANY], out_specs=specs,
        scratch_shapes=[pltpu.VMEM((3, dim, HB), F32), pltpu.VMEM((3, HB, dim), F32), pltpu.VMEM((3, rows, HB), F32),
                        pltpu.VMEM((3, rows, HB), BF16), pltpu.VMEM((HB, rows), BF16), pltpu.VMEM((HB, rows), BF16),
                        pltpu.VMEM((rows, HB), BF16), pltpu.VMEM((rows, HB), BF16),
                        pltpu.VMEM((NS, 2, HB, HB), BF16), pltpu.VMEM((NS, 2, HB, HB), BF16),
                        pltpu.VMEM((NS, 2, HB, HB), BF16), pltpu.VMEM((rows, dim), F32),
                        DMA((4, 3)), DMA((NS, 2)), DMA((NS, 2)), DMA((NS, 2))],
        compiler_params=pltpu.CompilerParams(collective_id=l, has_side_effects=True, vmem_limit_bytes=60 << 20),
        cost_estimate=pl.CostEstimate(flops=8 * rows * dim * hid, bytes_accessed=60 << 20, transcendentals=0),
        name='back')(v, d, r, w_up, w_down, slope, z)


def add_body(n, a_ref, b_ref, *refs):
    outs, (a, b, in_sem, out_sem) = refs[:-4], refs[-4:]
    order = list(range(n // 2, n)) + list(range(n // 2)) if n > 1 else [0]

    def copies(i):
        return (pltpu.make_async_copy(a_ref.at[i], a.at[i], in_sem.at[0, i]),
                pltpu.make_async_copy(b_ref.at[i], b.at[i], in_sem.at[1, i]))

    done = []
    for i in order:
        for c in copies(i):
            c.start()
    for i in order:
        for c in copies(i):
            c.wait()
        a[i] = add_bf(a[i], b[i])
        if n == 1:
            dst = outs[0].at[0]
        elif i >= n // 2:
            dst = outs[0].at[i - n // 2]
        else:
            dst = outs[1].at[i]
        c = pltpu.make_async_copy(a.at[i], dst, out_sem.at[i])
        c.start()
        done.append(c)
    for c in done:
        c.wait()


def add_halves(a, b):
    n = a.shape[0]
    out = jax.ShapeDtypeStruct((max(n // 2, 1), HB, HB), BF16)
    count = 2 if n > 1 else 1
    return pl.pallas_call(
        functools.partial(add_body, n), out_shape=[out] * count, in_specs=[ANY, ANY], out_specs=[ANY] * count,
        scratch_shapes=[pltpu.VMEM((n, HB, HB), BF16), pltpu.VMEM((n, HB, HB), BF16), DMA((2, n)), DMA((n,))],
        cost_estimate=pl.CostEstimate(flops=n << 29, bytes_accessed=3 * n << 19, transcendentals=0),
        name='add')(a, b)


def cat_body(a_ref, b_ref, o_ref, buf, in_sem, out_sem):
    n = a_ref.shape[0]
    loads = [pltpu.make_async_copy((a_ref if i < n else b_ref).at[i % n], buf.at[i], in_sem.at[i]) for i in range(2 * n)]
    stores = [pltpu.make_async_copy(buf.at[i], o_ref.at[i], out_sem.at[i]) for i in range(2 * n)]
    for c in loads:
        c.start()
    for c, d in zip(loads, stores):
        c.wait()
        d.start()
    for d in stores:
        d.wait()


def cat_halves(a, b):
    n = 2 * a.shape[0]
    return pl.pallas_call(
        cat_body, out_shape=jax.ShapeDtypeStruct((n, HB, HB), BF16), in_specs=[ANY, ANY], out_specs=ANY,
        scratch_shapes=[pltpu.VMEM((n, HB, HB), BF16), DMA((n,)), DMA((n,))],
        cost_estimate=pl.CostEstimate(flops=n << 29, bytes_accessed=2 * n << 19, transcendentals=0),
        name='cat')(a, b)


def fwd_body(l, r_ref, w1_ref, w2_ref, rn_ref, z_ref, slope_ref, w1, w2, act, zs, ss, in_sem, out_sem):
    def load(i):
        cols = pl.ds(pl.multiple_of(i * HB, HB), HB)
        return (pltpu.make_async_copy(w1_ref.at[l, :, cols], w1.at[i % 4], in_sem.at[0, i % 4]),
                pltpu.make_async_copy(w2_ref.at[l, cols, :], w2.at[i % 4], in_sem.at[1, i % 4]))

    def store(i):
        cols = pl.ds(pl.multiple_of(i * HB, HB), HB)
        return (pltpu.make_async_copy(zs.at[i % 3], z_ref.at[:, cols], out_sem.at[0, i % 3]),
                pltpu.make_async_copy(ss.at[i % 3], slope_ref.at[:, cols], out_sem.at[1, i % 3]))

    def first(i):
        hidden, slope = gelu_parts(dot(act[...], w1[i % 4].astype(BF16)))
        zs[i % 3] = hidden.astype(BF16)
        ss[i % 3] = slope

    def second(i):
        rn_ref[...] += dot(zs[i % 3], w2[i % 4].astype(BF16))

    for i in (0, 1, 2):
        for c in load(i):
            c.start()
    residual = r_ref[...]
    rn_ref[...] = residual
    act[...] = layer_norm(residual)[0].astype(BF16)
    load(0)[0].wait()
    first(0)
    for c in store(0):
        c.start()

    def step(i, _):
        load(i)[0].wait()
        load(i - 1)[1].wait()

        @pl.when(i >= 3)
        def _():
            for c in store(i - 3):
                c.wait()

        second(i - 1)
        first(i)
        for c in store(i):
            c.start()

        @pl.when(i + 2 < NB)
        def _():
            for c in load(i + 2):
                c.start()

        return 0

    lax.fori_loop(1, NB, step, 0)
    load(NB - 1)[1].wait()
    second(NB - 1)
    for i in range(NB - 3, NB):
        for c in store(i):
            c.wait()


def forward(l, r, w_up, w_down):
    rows, dim, hid = 512, 1024, 4096
    return pl.pallas_call(
        functools.partial(fwd_body, l),
        out_shape=[jax.ShapeDtypeStruct((rows, dim), F32), jax.ShapeDtypeStruct((rows, hid), BF16),
                   jax.ShapeDtypeStruct((rows, hid), F32)],
        in_specs=[WHOLE, ANY, ANY], out_specs=[WHOLE, ANY, ANY],
        scratch_shapes=[pltpu.VMEM((4, dim, HB), F32), pltpu.VMEM((4, HB, dim), F32), pltpu.VMEM((rows, dim), BF16),
                        pltpu.VMEM((3, rows, HB), BF16), pltpu.VMEM((3, rows, HB), F32), DMA((2, 4)), DMA((2, 3))],
        compiler_params=pltpu.CompilerParams(vmem_limit_bytes=48 << 20),
        cost_estimate=pl.CostEstimate(flops=4 * rows * dim * hid, bytes_accessed=46 << 20, transcendentals=0),
        name='forward')(r, w_up, w_down)


def update_body(l, k, kind, order, sc, into, rates_ref, *refs):
    acts = ()
    if kind == 'up':
        acts, refs = refs[:1], refs[1:]
    elif kind == 'down':
        acts, refs = refs[:2], refs[2:]
    pieces = 1 if sc else 4
    grads, refs = refs[:pieces], refs[pieces:]
    w_ref, m_ref = refs[:2]
    refs = refs[4:] if into else refs[2:]
    nw_ref, nm_ref, out_ref = refs[:3]
    w, m, g, ob, act, in_sem, g_sem, out_sem, ob_sem = refs[3:]
    _, _, chip, core = place()
    lr, mu = rates_ref[0], rates_ref[1]
    offs = (core * HB, (1 - core) * HB)

    def natural(i):
        cube = 0
        for s, v in enumerate(order):
            cube = cube + ((i // (4 >> s)) % 2) * v
        return flip(cube, chip)

    def at(i):
        span = pl.ds(pl.multiple_of(natural(i) * HB, HB), HB)
        return (l, slice(None), span) if k == 0 else (l, span, slice(None))

    def load(i, slot):
        out = [pltpu.make_async_copy(w_ref.at[at(i)], w.at[slot], in_sem.at[0, slot]),
               pltpu.make_async_copy(m_ref.at[at(i)], m.at[slot], in_sem.at[1, slot])]
        if kind == 'down':
            span = pl.ds(pl.multiple_of(natural(i) * HB, HB), HB)
            out.append(pltpu.make_async_copy(acts[1].at[:, span], act.at[slot], in_sem.at[2, slot]))
        return out

    def load_grad(i, slot, h, high):
        if sc:
            src = grads[0].at[natural(i) * 2 + (core if h == 0 else 1 - core)]
        else:
            src = grads[2 * h + high].at[i % 4]
        return pltpu.make_async_copy(src, g.at[slot, h], g_sem.at[slot, h])

    def start(i, slot):
        for c in load(i, slot):
            c.start()
        for h in (0, 1):
            if sc:
                load_grad(i, slot, h, 0).start()
                continue
            for high in (0, 1):
                @pl.when(i // 4 == high)
                def _():
                    load_grad(i, slot, h, high).start()

    def store(i, slot):
        return (pltpu.make_async_copy(w.at[slot], nw_ref.at[at(i)], out_sem.at[0, slot]),
                pltpu.make_async_copy(m.at[slot], nm_ref.at[at(i)], out_sem.at[1, slot]))

    def store_last(i):
        span = pl.ds(pl.multiple_of(natural(i) * HB, HB), HB)
        if kind == 'up':
            return pltpu.make_async_copy(ob.at[i % 2], out_ref.at[:, span], ob_sem.at[i % 2])
        dst = out_ref.at[:, span] if k == 0 else out_ref.at[span, :]
        return pltpu.make_async_copy(ob.at[i % 2], dst, ob_sem.at[i % 2])

    start(0, 0)
    start(1, 1)
    if kind == 'up':
        act[...] = layer_norm(acts[0][...])[0].astype(BF16)
    elif kind == 'down':
        out_ref[...] = acts[0][...]

    def step(i, _):
        slot = i % 4

        @pl.when(i + 2 < NB)
        def _():
            @pl.when(i >= 2)
            def _():
                for c in store(i - 2, (i + 2) % 4):
                    c.wait()

            start(i + 2, (i + 2) % 4)

        for c in load(i, slot):
            c.wait()
        for h in (0, 1):
            load_grad(i, slot, h, 0).wait()
            part = pl.ds(pl.multiple_of(offs[h], HB), HB)
            idx = (slot, part, slice(None)) if k == 0 else (slot, slice(None), part)
            new_m = mu * m[idx] + g[slot, h].astype(F32)
            m[idx] = new_m
            w[idx] = w[idx] - lr * new_m
        for c in store(i, slot):
            c.start()
        new_bf = w[slot].astype(BF16)
        if kind == 'down':
            out_ref[...] += dot(act[slot], new_bf)
        else:
            @pl.when(i >= 2)
            def _():
                store_last(i - 2).wait()

            if kind == 'up':
                ob[i % 2] = gelu(dot(act[...], new_bf)).astype(BF16)
            else:
                ob[i % 2] = new_bf
            store_last(i).start()
        return 0

    lax.fori_loop(0, NB, step, 0)
    for i in range(NB - 4, NB):
        for c in store(i, i % 4):
            c.wait()
    if kind != 'down':
        for i in range(NB - 2, NB):
            store_last(i).wait()


def update(m, kind, rates, acts, grads, w, mom, into):
    l, k = m
    dim, hid, rows = 1024, 4096, 512
    sc = len(grads) == 1
    wide = (dim, HB) if k == 0 else (HB, dim)
    if kind == 'up':
        act_specs, last, last_spec = [WHOLE], jax.ShapeDtypeStruct((rows, hid), BF16), ANY
        ob, act = (2, rows, HB), (rows, dim)
    elif kind == 'down':
        act_specs, last, last_spec = [WHOLE, ANY], jax.ShapeDtypeStruct((rows, dim), F32), WHOLE
        ob, act = (2, 16, 128), (4, rows, HB)
    else:
        act_specs, last_spec = [], ANY
        last = jax.ShapeDtypeStruct((dim, hid) if k == 0 else (hid, dim), BF16)
        ob, act = (2,) + wide, (16, 128)
    in_specs = [pl.BlockSpec(memory_space=pltpu.SMEM)] + act_specs + [ANY] * (len(grads) + 2)
    args = [rates, *acts, *grads, w, mom]
    aliases = {}
    if into is not None:
        aliases = {len(args): 0, len(args) + 1: 1}
        in_specs += [ANY, ANY]
        args += list(into)
    full = jax.ShapeDtypeStruct(w.shape, F32)
    return pl.pallas_call(
        functools.partial(update_body, l, k, kind, order_of(m), sc, into is not None),
        out_shape=[full, full, last], in_specs=in_specs, out_specs=[ANY, ANY, last_spec],
        scratch_shapes=[pltpu.VMEM((4,) + wide, F32), pltpu.VMEM((4,) + wide, F32), pltpu.VMEM((4, 2, HB, HB), BF16),
                        pltpu.VMEM(ob, BF16), pltpu.VMEM(act, BF16),
                        DMA((3, 4)), DMA((4, 2)), DMA((2, 4)), DMA((2,))],
        input_output_aliases=aliases,
        compiler_params=pltpu.CompilerParams(vmem_limit_bytes=48 << 20),
        cost_estimate=pl.CostEstimate(flops=10_000_000_000, bytes_accessed=80 << 20, transcendentals=0))(*args)


def solution(mesh):
    num_dev = mesh.shape['rep'] * mesh.shape['data']
    pairs = {v: [(i, i ^ max(2 * v, 1)) for i in range(num_dev)] for v in (0, 1, 2, 4)}

    def local_step(x_now, x_next, labels, w_up, w_down, w_head, mom_up, mom_down, mom_head, learn_rate, momentum):
        images, seq_len, model_dim = x_now.shape
        layers = w_up.shape[0]
        classes = w_head.shape[1]
        rows = images * seq_len
        global_batch = images * num_dev
        weights = (w_up, w_down)
        moms = (mom_up, mom_down)
        rates = jnp.stack([learn_rate, momentum])
        token = [None]

        def hold(*args):
            if token[0] is None:
                return args
            return lax.optimization_barrier((*args, token[0]))[:-1]

        def cp(x, link):
            return lax.ppermute(x, BATCH_AXES, pairs[link])

        residual = x_now.reshape(rows, model_dim).astype(F32)
        saved = []
        for l in range(layers):
            after, hid_bf, slope = forward(l, residual, w_up, w_down)
            saved.append((residual, slope, hid_bf))
            residual = after
        head_bf = w_head.astype(BF16)
        pooled, logits = pool_logits(residual, images, head_bf)
        soft_probs = jax.nn.softmax(logits, axis=-1)
        onehot = (labels[:, None] == jnp.arange(classes, dtype=jnp.int32)[None, :]).astype(F32)
        d_logits = ((soft_probs - onehot) / global_batch).astype(BF16)
        grad_head = jnp.einsum('bd,bc->dc', pooled, d_logits, preferred_element_type=F32)
        red_head = lax.psum(grad_head.astype(BF16), BATCH_AXES)
        d_pooled = jnp.einsum('bc,dc->bd', d_logits, head_bf, preferred_element_type=F32)
        d_resid = jnp.broadcast_to((d_pooled / seq_len)[:, None, :], (images, seq_len, model_dim)).reshape(rows, model_dim)

        d_res, v_bf = d_resid, d_resid.astype(BF16)
        box = {}
        new = [None, None]
        res_next = {0: x_next.reshape(rows, model_dim).astype(F32)}
        z_next = {}
        w_bf = {}

        def step(op, l, k):
            nonlocal d_res, v_bf
            m = (l, k)
            order = order_of(m)
            if op == 'B':
                v, d, r = hold(v_bf, d_res, saved[l][0])
                out = back(l, v, d, r, w_up, w_down, saved[l][1], saved[l][2])
                for j in (1, 0):
                    box['s1', (l, j)], box['k1', (l, j)] = out[2 * j], out[2 * j + 1]
                if l > 0:
                    d_res, v_bf = out[4:]
                out = out[3]
            elif op == 'a':
                send, = hold(box.pop(('s1', m)))
                box['r1', m] = cp(send, order[0])
                return
            elif op in 'bc':
                src, dst = {'b': ('1', '2'), 'c': ('2', '3')}[op]
                keep, got = hold(box.pop(('k' + src, m)), box.pop(('r' + src, m)))
                out, box['k' + dst, m] = add_halves(keep, got)
                box['r' + dst, m] = cp(out, order[1] if op == 'b' else order[2])
                out = box['k' + dst, m]
            elif op == 'd':
                keep, got = hold(box.pop(('k3', m)), box.pop(('r3', m)))
                out, = add_halves(keep, got)
                if m in GATHER_SC:
                    box['g', m] = (lax.all_gather(out, BATCH_AXES).reshape(num_dev, HB, HB),)
                else:
                    box['p0', m] = out
                    box['q0', m] = cp(out, order[2])
            elif op in 'ef':
                src, dst = {'e': ('0', '1'), 'f': ('1', '2')}[op]
                own, got = hold(box.pop(('p' + src, m)), box.pop(('q' + src, m)))
                out = cat_halves(own, got)
                if op == 'e':
                    box['p1', m] = out
                    box['q1', m] = cp(out, order[1])
                else:
                    far = cp(out, order[0])
                    box['g', m] = (out, far, cp(out, 0))
            elif op == 'h':
                own, far, other = box['g', m]
                send, = hold(far)
                box['g', m] = (own, far, other, cp(send, 0))
                return
            elif op in 'KU':
                kind = 'plain' if op == 'U' else ('up' if k == 0 else 'down')
                acts = ()
                if kind == 'up':
                    acts = (res_next[l],)
                elif kind == 'down':
                    acts = (res_next[l], z_next[l])
                held = hold(*acts, *box.pop(('g', m)))
                acts, grads = held[:len(acts)], held[len(acts):]
                nw, nm, out = update(m, kind, rates, acts, grads, weights[k], moms[k], new[k])
                new[k] = (nw, nm)
                if kind == 'up':
                    z_next[l] = out
                elif kind == 'down':
                    res_next[l + 1] = out
                else:
                    w_bf[m] = out
            elif op == 'F':
                if k == 0:
                    r, w = hold(res_next[l], w_bf[m])
                    out = gelu(jnp.dot(layer_norm(r)[0].astype(BF16), w, preferred_element_type=F32)).astype(BF16)
                    z_next[l] = out
                else:
                    r, z, w = hold(res_next[l], z_next[l], w_bf[m])
                    out = r + jnp.dot(z, w, preferred_element_type=F32)
                    res_next[l + 1] = out
            elif op == 'H':
                red, mh, wh = hold(red_head, mom_head, w_head)
                nm = momentum * mh + red.astype(F32)
                nw = wh - learn_rate * nm
                box['head'] = (nw, nm)
                out = nm
            token[0] = out

        for op, l, k in ORDER:
            step(op, l, k)
        new_head, new_mom_head = box['head']
        _, logits_next = pool_logits(res_next[layers], images, new_head.astype(jnp.bfloat16))
        return logits_next, new[0][0], new[1][0], new_head, new[0][1], new[1][1], new_mom_head

    batch_spec = P(BATCH_AXES)
    whole_spec = P()
    return jax.shard_map(local_step, mesh=mesh,
                         in_specs=(batch_spec, batch_spec, batch_spec) + (whole_spec,) * 8,
                         out_specs=(batch_spec,) + (whole_spec,) * 6,
                         check_vma=False)
```

```python
import functools

import jax
import jax.numpy as jnp
from jax import lax
from jax.experimental import pallas as pl
from jax.experimental.pallas import tpu as pltpu
from jax.sharding import PartitionSpec as P


LN_EPS = 1e-6
BATCH_AXES = ('rep', 'data')
NB = 8
HB = 512
NS = 4
LINKS = (1, 2, 4)
ADMIT = ((5, 1), (5, 0), (4, 1), (3, 1), (4, 0), (1, 0), (2, 0), (1, 1), (0, 0), (0, 1), (2, 1), (3, 0),)
GATHER_SC = ((0, 0), (0, 1), (2, 1), (3, 0),)
ORDER = tuple((t[0], int(t[1]), int(t[2])) for t in (
    'B50', 'a51', 'a50', 'B40', 'a41', 'B30', 'a31', 'a40', 'b50', 'b51', 'B20', 'b41',
    'c50', 'b31', 'b40', 'B10', 'c51', 'd50', 'a10', 'c41', 'c31', 'c40', 'd51', 'a20',
    'e50', 'd41', 'a11', 'B00', 'd40', 'a00', 'e41', 'b10', 'H00', 'b20', 'd31', 'a01',
    'e51', 'e40', 'b11', 'f50', 'f41', 'c20', 'c10', 'f51', 'b00', 'e31', 'b01', 'h50',
    'f40', 'd10', 'a21', 'U50', 'c11', 'h51', 'f31', 'U51', 'c01', 'd11', 'a30', 'd20',
    'c00', 'h41', 'd01', 'h40', 'U41', 'h31', 'e10', 'U40', 'b30', 'e20', 'b21', 'e11',
    'd00', 'U31', 'f10', 'c30', 'c21', 'U01', 'f20', 'f11', 'd21', 'K00', 'd30', 'F01',
    'h20', 'h10', 'h11', 'K10', 'K11', 'K20', 'K21', 'K30', 'F31', 'F40', 'F41', 'F50',
    'F51',
))


def layer_norm(residual):
    centered = residual - jnp.mean(residual, axis=-1, keepdims=True)
    inv_std = lax.rsqrt(jnp.mean(centered * centered, axis=-1, keepdims=True) + LN_EPS)
    return centered * inv_std, inv_std


def norm_back(normed, inv_std, grad_out):
    return inv_std * (grad_out - jnp.mean(grad_out, axis=-1, keepdims=True)
                      - normed * jnp.mean(grad_out * normed, axis=-1, keepdims=True))


def gelu(pre_act):
    return pre_act * (0.5 * (1.0 + lax.erf(pre_act * 0.7071067811865476)))


def gelu_parts(pre_act):
    gauss_cdf = 0.5 * (1.0 + lax.erf(pre_act * 0.7071067811865476))
    density = jnp.exp(-0.5 * pre_act * pre_act) * 0.3989422804014327
    return pre_act * gauss_cdf, gauss_cdf + pre_act * density


def pool_logits(residual, images, head_bf):
    pooled = jnp.mean(residual.reshape(images, -1, residual.shape[-1]), axis=1).astype(jnp.bfloat16)
    return pooled, jnp.dot(pooled, head_bf, preferred_element_type=jnp.float32)


def order_of(m):
    i = ADMIT.index(m) % 3
    return tuple(LINKS[(i + s) % 3] for s in range(3))


def unmask(block, order):
    return ((block // order[0]) % 2) * 4 + ((block // order[1]) % 2) * 2 + (block // order[2]) % 2


def flip(a, b):
    out = 0
    for v in (1, 2, 4):
        x, y = (a // v) % 2, (b // v) % 2
        out = out + (x + y - 2 * x * y) * v
    return out


def place():
    rep, data = lax.axis_index('rep'), lax.axis_index('data')
    return rep, data, rep * 2 + data // 2, data % 2


def dot(a, b, ca=1, cb=0):
    return lax.dot_general(a, b, (((ca,), (cb,)), ((), ())), preferred_element_type=jnp.float32)


def add_bf(a, b):
    return (a.astype(jnp.float32) + b.astype(jnp.float32)).astype(jnp.bfloat16)


ANY = pl.BlockSpec(memory_space=pl.ANY)
WHOLE = pl.BlockSpec(memory_space=pltpu.VMEM)
DMA = pltpu.SemaphoreType.DMA
F32, BF16 = jnp.float32, jnp.bfloat16


def back_body(l, last, order_up, order_down, v_hbm, d_hbm, r_hbm, w1_ref, w2_ref, slope_ref, z_ref, *refs):
    up_s, up_k, down_s, down_k = refs[:4]
    refs = refs[4:]
    if not last:
        dn_hbm, vn_hbm = refs[:2]
        refs = refs[2:]
    (w1, w2, sl, zb, v_ref, d_ref, r_ref, at_own, at_far, v_own, v_far, mine, far, got, acc,
     in_sem, one_sem, out_sem, send_sem, recv_sem) = refs
    rep, data, chip, core = place()
    peer = (rep, data + 1 - 2 * core)
    barrier = pltpu.get_barrier_semaphore()

    def load(i, slot):
        cols = pl.ds(pl.multiple_of(i * HB, HB), HB)
        return (pltpu.make_async_copy(w2_ref.at[l, cols, :], w2.at[slot], in_sem.at[0, slot]),
                pltpu.make_async_copy(slope_ref.at[l, :, cols], sl.at[slot], in_sem.at[1, slot]),
                pltpu.make_async_copy(z_ref.at[l, :, cols], zb.at[slot], in_sem.at[2, slot]),
                pltpu.make_async_copy(w1_ref.at[l, :, cols], w1.at[slot], in_sem.at[3, slot]))

    def start(i, slot):
        for copy in load(i, slot):
            copy.start()

    def remote(i, k):
        return pltpu.make_async_remote_copy(
            src_ref=far.at[i % NS, k], dst_ref=got.at[i % NS, k],
            send_sem=send_sem.at[i % NS, k], recv_sem=recv_sem.at[i % NS, k],
            device_id=peer, device_id_type=pl.DeviceIdType.MESH)

    def stores(i):
        block = flip(i, chip)
        out = []
        for k, (os, ok, order) in enumerate(((up_s, up_k, order_up), (down_s, down_k, order_down))):
            pos = unmask(block, order)
            out.append((pos // 4, pltpu.make_async_copy(mine.at[i % NS, k], os.at[pos % 4], out_sem.at[i % NS, k]),
                        pltpu.make_async_copy(mine.at[i % NS, k], ok.at[pos % 4], out_sem.at[i % NS, k])))
        return out

    def finish(i):
        for k in (0, 1):
            remote(i, k).wait_recv()
            mine[i % NS, k] = add_bf(mine[i % NS, k], got[i % NS, k])
        for high, to_send, to_keep in stores(i):
            @pl.when(high == 1)
            def _():
                to_send.start()

            @pl.when(high == 0)
            def _():
                to_keep.start()

    def settle(i):
        for k in (0, 1):
            remote(i, k).wait_send()
        for high, to_send, to_keep in stores(i):
            @pl.when(high == 1)
            def _():
                to_send.wait()

            @pl.when(high == 0)
            def _():
                to_keep.wait()

    pl.semaphore_signal(barrier, inc=1, device_id=peer, device_id_type=pl.DeviceIdType.MESH)
    get_v = pltpu.make_async_copy(v_hbm, v_ref, one_sem.at[0])
    get_r = pltpu.make_async_copy(r_hbm.at[l], r_ref, one_sem.at[1])
    get_r.start()
    get_v.start()
    start(0, 0)
    start(1, 1)
    if not last:
        get_d = pltpu.make_async_copy(d_hbm, d_ref, one_sem.at[2])
        get_d.start()
    get_r.wait()
    residual = r_ref[...]
    normed, inv_std = layer_norm(residual)
    a_t = normed.astype(BF16).T
    own, other = pl.ds(pl.multiple_of(core * HB, HB), HB), pl.ds(pl.multiple_of((1 - core) * HB, HB), HB)
    acc[...] = jnp.zeros_like(acc)
    at_own[...] = a_t[:HB]
    at_far[...] = a_t[HB:]
    get_v.wait()
    v_own[...] = v_ref[:, own]
    v_far[...] = v_ref[:, other]

    @pl.when(core == 1)
    def _():
        tmp = at_own[...]
        at_own[...] = at_far[...]
        at_far[...] = tmp

    pl.semaphore_wait(barrier, 1)

    def step(i, _):
        slot = i % 3

        @pl.when(i + 2 < NB)
        def _():
            start(i + 2, (i + 2) % 3)

        @pl.when(i >= NS)
        def _():
            settle(i - NS)

        copies = load(i, slot)
        copies[0].wait()
        copies[1].wait()
        s = (dot(v_ref[...], w2[slot].astype(BF16), 1, 1) * sl[slot]).astype(BF16)
        far[i % NS, 0] = dot(at_far[...], s).astype(BF16)
        remote(i, 0).start()
        copies[2].wait()
        z_t = zb[slot].T
        far[i % NS, 1] = dot(z_t, v_far[...]).astype(BF16)
        remote(i, 1).start()
        mine[i % NS, 0] = dot(at_own[...], s).astype(BF16)
        mine[i % NS, 1] = dot(z_t, v_own[...]).astype(BF16)
        copies[3].wait()
        if not last:
            acc[...] += dot(s, w1[slot].astype(BF16), 1, 1)

        @pl.when(i > 0)
        def _():
            finish(i - 1)

        return 0

    lax.fori_loop(0, NB, step, 0)
    if not last:
        get_d.wait()
        residual = r_ref[...]
        normed, inv_std = layer_norm(residual)
        grad = d_ref[...] + norm_back(normed, inv_std, acc[...])
        d_ref[...] = grad
        v_ref[...] = grad.astype(BF16)
        put_d = pltpu.make_async_copy(d_ref, dn_hbm, one_sem.at[2])
        put_v = pltpu.make_async_copy(v_ref, vn_hbm, one_sem.at[0])
        put_d.start()
        put_v.start()
    finish(NB - 1)
    for i in range(NB - NS, NB):
        settle(i)
    if not last:
        put_d.wait()
        put_v.wait()


def back(l, v, d, r, w_up, w_down, slope, z):
    rows, dim, hid = 512, 1024, 4096
    last = l == 0
    tile = jax.ShapeDtypeStruct((4, HB, HB), BF16)
    outs, specs = [tile] * 4, [ANY] * 4
    if not last:
        outs += [jax.ShapeDtypeStruct((rows, dim), F32), jax.ShapeDtypeStruct((rows, dim), BF16)]
        specs += [ANY, ANY]
    return pl.pallas_call(
        functools.partial(back_body, l, last, order_of((l, 0)), order_of((l, 1))),
        out_shape=outs, in_specs=[ANY] * 7, out_specs=specs,
        scratch_shapes=[pltpu.VMEM((3, dim, HB), F32), pltpu.VMEM((3, HB, dim), F32), pltpu.VMEM((3, rows, HB), F32),
                        pltpu.VMEM((3, rows, HB), BF16), pltpu.VMEM((rows, dim), BF16), pltpu.VMEM((rows, dim), F32),
                        pltpu.VMEM((rows, dim), F32), pltpu.VMEM((HB, rows), BF16), pltpu.VMEM((HB, rows), BF16),
                        pltpu.VMEM((rows, HB), BF16), pltpu.VMEM((rows, HB), BF16),
                        pltpu.VMEM((NS, 2, HB, HB), BF16), pltpu.VMEM((NS, 2, HB, HB), BF16),
                        pltpu.VMEM((NS, 2, HB, HB), BF16), pltpu.VMEM((rows, dim), F32),
                        DMA((4, 3)), DMA((3,)), DMA((NS, 2)), DMA((NS, 2)), DMA((NS, 2))],
        compiler_params=pltpu.CompilerParams(collective_id=l, has_side_effects=True, vmem_limit_bytes=60 << 20),
        cost_estimate=pl.CostEstimate(flops=8 * rows * dim * hid, bytes_accessed=60 << 20, transcendentals=0),
        name='back')(v, d, r, w_up, w_down, slope, z)


def add_body(n, a_ref, b_ref, *refs):
    outs, (a, b, in_sem, out_sem) = refs[:-4], refs[-4:]
    order = list(range(n // 2, n)) + list(range(n // 2)) if n > 1 else [0]

    def copies(i):
        return (pltpu.make_async_copy(a_ref.at[i], a.at[i], in_sem.at[0, i]),
                pltpu.make_async_copy(b_ref.at[i], b.at[i], in_sem.at[1, i]))

    done = []
    for i in order:
        for c in copies(i):
            c.start()
    for i in order:
        for c in copies(i):
            c.wait()
        a[i] = add_bf(a[i], b[i])
        if n == 1:
            dst = outs[0].at[0]
        elif i >= n // 2:
            dst = outs[0].at[i - n // 2]
        else:
            dst = outs[1].at[i]
        c = pltpu.make_async_copy(a.at[i], dst, out_sem.at[i])
        c.start()
        done.append(c)
    for c in done:
        c.wait()


def add_halves(a, b):
    n = a.shape[0]
    out = jax.ShapeDtypeStruct((max(n // 2, 1), HB, HB), BF16)
    count = 2 if n > 1 else 1
    return pl.pallas_call(
        functools.partial(add_body, n), out_shape=[out] * count, in_specs=[ANY, ANY], out_specs=[ANY] * count,
        scratch_shapes=[pltpu.VMEM((n, HB, HB), BF16), pltpu.VMEM((n, HB, HB), BF16), DMA((2, n)), DMA((n,))],
        cost_estimate=pl.CostEstimate(flops=n << 29, bytes_accessed=3 * n << 19, transcendentals=0),
        name='add')(a, b)


def cat_body(a_ref, b_ref, o_ref, buf, in_sem, out_sem):
    n = a_ref.shape[0]
    loads = [pltpu.make_async_copy((a_ref if i < n else b_ref).at[i % n], buf.at[i], in_sem.at[i]) for i in range(2 * n)]
    stores = [pltpu.make_async_copy(buf.at[i], o_ref.at[i], out_sem.at[i]) for i in range(2 * n)]
    for c in loads:
        c.start()
    for c, d in zip(loads, stores):
        c.wait()
        d.start()
    for d in stores:
        d.wait()


def cat_halves(a, b):
    n = 2 * a.shape[0]
    return pl.pallas_call(
        cat_body, out_shape=jax.ShapeDtypeStruct((n, HB, HB), BF16), in_specs=[ANY, ANY], out_specs=ANY,
        scratch_shapes=[pltpu.VMEM((n, HB, HB), BF16), DMA((n,)), DMA((n,))],
        cost_estimate=pl.CostEstimate(flops=n << 29, bytes_accessed=2 * n << 19, transcendentals=0),
        name='cat')(a, b)


def fwd_body(layers, x_ref, w1_ref, w2_ref, rs_ref, z_ref, slope_ref, w1, w2, res, keep, act, zs, ss, in_sem, out_sem, res_sem):
    total = layers * NB

    def load(t):
        l, cols = t // NB, pl.ds(pl.multiple_of((t % NB) * HB, HB), HB)
        return (pltpu.make_async_copy(w1_ref.at[l, :, cols], w1.at[t % 4], in_sem.at[0, t % 4]),
                pltpu.make_async_copy(w2_ref.at[l, cols, :], w2.at[t % 4], in_sem.at[1, t % 4]))

    def store(t):
        l, cols = t // NB, pl.ds(pl.multiple_of((t % NB) * HB, HB), HB)
        return (pltpu.make_async_copy(zs.at[t % 3], z_ref.at[l, :, cols], out_sem.at[0, t % 3]),
                pltpu.make_async_copy(ss.at[t % 3], slope_ref.at[l, :, cols], out_sem.at[1, t % 3]))

    def store_res(l):
        return pltpu.make_async_copy(keep.at[l % 2], rs_ref.at[l], res_sem.at[l % 2])

    def prefetch(t):
        @pl.when(t < total)
        def _():
            for c in load(t):
                c.start()

    def first(t):
        @pl.when(t >= 3)
        def _():
            for c in store(t - 3):
                c.wait()

        hidden, slope = gelu_parts(dot(act[...], w1[t % 4].astype(BF16)))
        zs[t % 3] = hidden.astype(BF16)
        ss[t % 3] = slope
        for c in store(t):
            c.start()

    def second(t):
        res[...] += dot(zs[t % 3], w2[t % 4].astype(BF16))

    for t in (0, 1, 2):
        for c in load(t):
            c.start()
    res[...] = x_ref[...].astype(F32)

    def block(l, _):
        t0 = l * NB

        @pl.when(l >= 2)
        def _():
            store_res(l - 2).wait()

        residual = res[...]
        keep[l % 2] = residual
        store_res(l).start()
        act[...] = layer_norm(residual)[0].astype(BF16)
        load(t0)[0].wait()
        first(t0)

        def step(i, _):
            t = t0 + i
            prefetch(t + 2)
            load(t)[0].wait()
            load(t - 1)[1].wait()

            @pl.when(t >= 3)
            def _():
                for c in store(t - 3):
                    c.wait()

            res[...] += dot(zs[(t - 1) % 3], w2[(t - 1) % 4].astype(BF16))
            hidden, slope = gelu_parts(dot(act[...], w1[t % 4].astype(BF16)))
            zs[t % 3] = hidden.astype(BF16)
            ss[t % 3] = slope
            for c in store(t):
                c.start()
            return 0

        lax.fori_loop(1, NB, step, 0)
        load(t0 + NB - 1)[1].wait()
        second(t0 + NB - 1)
        prefetch(t0 + NB + 2)
        return 0

    lax.fori_loop(0, layers, block, 0)

    store_res(layers - 2).wait()
    keep[layers % 2] = res[...]
    store_res(layers).start()
    for t in range(total - 3, total):
        for c in store(t):
            c.wait()
    for l in (layers - 1, layers):
        store_res(l).wait()


def forward(x, w_up, w_down):
    rows, dim, hid, layers = 512, 1024, 4096, 6
    return pl.pallas_call(
        functools.partial(fwd_body, layers),
        out_shape=[jax.ShapeDtypeStruct((layers + 1, rows, dim), F32), jax.ShapeDtypeStruct((layers, rows, hid), BF16),
                   jax.ShapeDtypeStruct((layers, rows, hid), F32)],
        in_specs=[WHOLE, ANY, ANY], out_specs=[ANY, ANY, ANY],
        scratch_shapes=[pltpu.VMEM((4, dim, HB), F32), pltpu.VMEM((4, HB, dim), F32), pltpu.VMEM((rows, dim), F32),
                        pltpu.VMEM((2, rows, dim), F32), pltpu.VMEM((rows, dim), BF16), pltpu.VMEM((3, rows, HB), BF16),
                        pltpu.VMEM((3, rows, HB), F32), DMA((2, 4)), DMA((2, 3)), DMA((2,))],
        compiler_params=pltpu.CompilerParams(vmem_limit_bytes=50 << 20),
        cost_estimate=pl.CostEstimate(flops=24 * rows * dim * hid, bytes_accessed=280 << 20, transcendentals=0),
        name='forward')(x, w_up, w_down)


def update_body(l, k, kind, order, sc, into, rates_ref, *refs):
    acts = ()
    if kind == 'up':
        acts, refs = refs[:1], refs[1:]
    elif kind == 'down':
        acts, refs = refs[:2], refs[2:]
    pieces = 1 if sc else 4
    grads, refs = refs[:pieces], refs[pieces:]
    w_ref, m_ref = refs[:2]
    refs = refs[4:] if into else refs[2:]
    nw_ref, nm_ref, out_ref = refs[:3]
    w, m, g, ob, act, in_sem, act_sem, out_sem, ob_sem = refs[3:]
    _, _, chip, core = place()
    lr, mu = rates_ref[0], rates_ref[1]
    sides = [pl.ds(pl.multiple_of(core * HB, HB), HB), pl.ds(pl.multiple_of((1 - core) * HB, HB), HB)]
    slots = 6

    def natural(i):
        cube = 0
        for s, v in enumerate(order):
            cube = cube + ((i // (4 >> s)) % 2) * v
        return flip(cube, chip)

    def span(i):
        return pl.ds(pl.multiple_of(natural(i) * HB, HB), HB)

    def at(i, h):
        return (l, sides[h], span(i)) if k == 0 else (l, span(i), sides[h])

    def load(i, h):
        slot = (2 * i + h) % slots
        return (pltpu.make_async_copy(w_ref.at[at(i, h)], w.at[slot], in_sem.at[0, slot]),
                pltpu.make_async_copy(m_ref.at[at(i, h)], m.at[slot], in_sem.at[1, slot]))

    def load_act(i):
        return pltpu.make_async_copy(acts[1].at[:, span(i)], act.at[i % 3], act_sem.at[i % 3])

    def load_grad(i, h, high):
        slot = (2 * i + h) % slots
        src = grads[0].at[natural(i) * 2 + (core if h == 0 else 1 - core)] if sc else grads[2 * h + high].at[i % 4]
        return pltpu.make_async_copy(src, g.at[slot], in_sem.at[2, slot])

    def start(i, h):
        for c in load(i, h):
            c.start()
        if kind == 'down' and h == 0:
            load_act(i).start()
        if sc:
            load_grad(i, h, 0).start()
            return
        for high in (0, 1):
            @pl.when(i // 4 == high)
            def _():
                load_grad(i, h, high).start()

    def store(i, h):
        slot = (2 * i + h) % slots
        return (pltpu.make_async_copy(w.at[slot], nw_ref.at[at(i, h)], out_sem.at[0, slot]),
                pltpu.make_async_copy(m.at[slot], nm_ref.at[at(i, h)], out_sem.at[1, slot]))

    def store_last(i, h):
        if kind == 'up':
            return pltpu.make_async_copy(ob.at[i % 2], out_ref.at[:, span(i)], ob_sem.at[i % 2])
        return pltpu.make_async_copy(ob.at[i % 2, h], out_ref.at[at(i, h)[1:]], ob_sem.at[i % 2, h])

    def whole_last(i):
        return (store_last(i, 0),) if kind == 'up' else (store_last(i, 0), store_last(i, 1))

    start(0, 0)
    start(0, 1)
    start(1, 0)
    if kind == 'up':
        residual = acts[0][...]
        normed = layer_norm(residual)[0].astype(BF16)
        act[...] = normed
    elif kind == 'down':
        out_ref[...] = acts[0][...]

    def step(i, _):
        pre = None
        if kind != 'down':
            @pl.when(i >= 2)
            def _():
                for c in whole_last(i - 2):
                    c.wait()
        for h in (0, 1):
            slot = (2 * i + h) % slots
            ahead, side = (i + 1, 1) if h == 0 else (i + 2, 0)
            back_i, back_h = (i - 2, 1) if h == 0 else (i - 1, 0)

            @pl.when(ahead < NB)
            def _():
                @pl.when(back_i >= 0)
                def _():
                    for c in store(back_i, back_h):
                        c.wait()

                start(ahead, side)

            for c in load(i, h):
                c.wait()
            load_grad(i, h, 0).wait()
            new_m = mu * m[slot] + g[slot].astype(F32)
            new_w = w[slot] - lr * new_m
            m[slot] = new_m
            w[slot] = new_w
            for c in store(i, h):
                c.start()
            new_bf = new_w.astype(BF16)
            if kind == 'up':
                part = dot(act[:, sides[h]], new_bf)
                pre = part if h == 0 else pre + part
            elif kind == 'down':
                if h == 0:
                    load_act(i).wait()
                out_ref[:, sides[h]] += dot(act[i % 3], new_bf)
            else:
                ob[i % 2, h] = new_bf
        if kind == 'up':
            ob[i % 2] = gelu(pre).astype(BF16)
        if kind != 'down':
            for c in whole_last(i):
                c.start()
        return 0

    lax.fori_loop(0, NB, step, 0)
    for s in range(2 * NB - 6, 2 * NB):
        for c in store(s // 2, s % 2):
            c.wait()
    if kind != 'down':
        for i in range(NB - 2, NB):
            for c in whole_last(i):
                c.wait()


def update(m, kind, rates, acts, grads, w, mom, into):
    l, k = m
    dim, hid, rows = 1024, 4096, 512
    sc = len(grads) == 1
    ob_sem = DMA((2,))
    if kind == 'up':
        act_specs, last, last_spec = [WHOLE], jax.ShapeDtypeStruct((rows, hid), BF16), ANY
        ob, act = (2, rows, HB), (rows, dim)
    elif kind == 'down':
        act_specs, last, last_spec = [WHOLE, ANY], jax.ShapeDtypeStruct((rows, dim), F32), WHOLE
        ob, act = (2, 16, 128), (3, rows, HB)
    else:
        act_specs, last_spec = [], ANY
        last = jax.ShapeDtypeStruct((dim, hid) if k == 0 else (hid, dim), BF16)
        ob, act = (2, 2, HB, HB), (16, 128)
        ob_sem = DMA((2, 2))
    in_specs = [pl.BlockSpec(memory_space=pltpu.SMEM)] + act_specs + [ANY] * (len(grads) + 2)
    args = [rates, *acts, *grads, w, mom]
    aliases = {}
    if into is not None:
        aliases = {len(args): 0, len(args) + 1: 1}
        in_specs += [ANY, ANY]
        args += list(into)
    full = jax.ShapeDtypeStruct(w.shape, F32)
    return pl.pallas_call(
        functools.partial(update_body, l, k, kind, order_of(m), sc, into is not None),
        out_shape=[full, full, last], in_specs=in_specs, out_specs=[ANY, ANY, last_spec],
        scratch_shapes=[pltpu.VMEM((6, HB, HB), F32), pltpu.VMEM((6, HB, HB), F32), pltpu.VMEM((6, HB, HB), BF16),
                        pltpu.VMEM(ob, BF16), pltpu.VMEM(act, BF16),
                        DMA((3, 6)), DMA((3,)), DMA((2, 6)), ob_sem],
        input_output_aliases=aliases,
        compiler_params=pltpu.CompilerParams(vmem_limit_bytes=48 << 20),
        cost_estimate=pl.CostEstimate(flops=10_000_000_000, bytes_accessed=80 << 20, transcendentals=0))(*args)


def solution(mesh):
    num_dev = mesh.shape['rep'] * mesh.shape['data']
    pairs = {v: [(i, i ^ max(2 * v, 1)) for i in range(num_dev)] for v in (0, 1, 2, 4)}

    def local_step(x_now, x_next, labels, w_up, w_down, w_head, mom_up, mom_down, mom_head, learn_rate, momentum):
        images, seq_len, model_dim = x_now.shape
        layers = w_up.shape[0]
        classes = w_head.shape[1]
        rows = images * seq_len
        global_batch = images * num_dev
        weights = (w_up, w_down)
        moms = (mom_up, mom_down)
        rates = jnp.stack([learn_rate, momentum])
        token = [None]

        def hold(*args):
            if token[0] is None:
                return args
            return lax.optimization_barrier((*args, token[0]))[:-1]

        def cp(x, link):
            return lax.ppermute(x, BATCH_AXES, pairs[link])

        stream, hidden, slopes = forward(x_now.reshape(rows, model_dim), w_up, w_down)
        residual = stream[layers]
        head_bf = w_head.astype(BF16)
        pooled, logits = pool_logits(residual, images, head_bf)
        soft_probs = jax.nn.softmax(logits, axis=-1)
        onehot = (labels[:, None] == jnp.arange(classes, dtype=jnp.int32)[None, :]).astype(F32)
        d_logits = ((soft_probs - onehot) / global_batch).astype(BF16)
        grad_head = jnp.einsum('bd,bc->dc', pooled, d_logits, preferred_element_type=F32)
        red_head = lax.psum(grad_head.astype(BF16), BATCH_AXES)
        d_pooled = jnp.einsum('bc,dc->bd', d_logits, head_bf, preferred_element_type=F32)
        d_resid = jnp.broadcast_to((d_pooled / seq_len)[:, None, :], (images, seq_len, model_dim)).reshape(rows, model_dim)

        d_res, v_bf = d_resid, d_resid.astype(BF16)
        box = {}
        new = [None, None]
        res_next = {0: x_next.reshape(rows, model_dim).astype(F32)}
        z_next = {}
        w_bf = {}

        def step(op, l, k):
            nonlocal d_res, v_bf
            m = (l, k)
            order = order_of(m)
            if op == 'B':
                v, d = hold(v_bf, d_res)
                out = back(l, v, d, stream, w_up, w_down, slopes, hidden)
                for j in (1, 0):
                    box['s1', (l, j)], box['k1', (l, j)] = out[2 * j], out[2 * j + 1]
                if l > 0:
                    d_res, v_bf = out[4:]
                out = out[3]
            elif op == 'a':
                send, = hold(box.pop(('s1', m)))
                box['r1', m] = cp(send, order[0])
                return
            elif op in 'bc':
                src, dst = {'b': ('1', '2'), 'c': ('2', '3')}[op]
                keep, got = hold(box.pop(('k' + src, m)), box.pop(('r' + src, m)))
                out, box['k' + dst, m] = add_halves(keep, got)
                box['r' + dst, m] = cp(out, order[1] if op == 'b' else order[2])
                out = box['k' + dst, m]
            elif op == 'd':
                keep, got = hold(box.pop(('k3', m)), box.pop(('r3', m)))
                out, = add_halves(keep, got)
                if m in GATHER_SC:
                    box['g', m] = (lax.all_gather(out, BATCH_AXES).reshape(num_dev, HB, HB),)
                else:
                    box['p0', m] = out
                    box['q0', m] = cp(out, order[2])
            elif op in 'ef':
                src, dst = {'e': ('0', '1'), 'f': ('1', '2')}[op]
                own, got = hold(box.pop(('p' + src, m)), box.pop(('q' + src, m)))
                out = cat_halves(own, got)
                if op == 'e':
                    box['p1', m] = out
                    box['q1', m] = cp(out, order[1])
                else:
                    far = cp(out, order[0])
                    box['g', m] = (out, far, cp(out, 0))
            elif op == 'h':
                own, far, other = box['g', m]
                send, = hold(far)
                box['g', m] = (own, far, other, cp(send, 0))
                return
            elif op in 'KU':
                kind = 'plain' if op == 'U' else ('up' if k == 0 else 'down')
                acts = ()
                if kind == 'up':
                    acts = (res_next[l],)
                elif kind == 'down':
                    acts = (res_next[l], z_next[l])
                held = hold(*acts, *box.pop(('g', m)))
                acts, grads = held[:len(acts)], held[len(acts):]
                nw, nm, out = update(m, kind, rates, acts, grads, weights[k], moms[k], new[k])
                new[k] = (nw, nm)
                if kind == 'up':
                    z_next[l] = out
                elif kind == 'down':
                    res_next[l + 1] = out
                else:
                    w_bf[m] = out
            elif op == 'F':
                if k == 0:
                    r, w = hold(res_next[l], w_bf[m])
                    out = gelu(jnp.dot(layer_norm(r)[0].astype(BF16), w, preferred_element_type=F32)).astype(BF16)
                    z_next[l] = out
                else:
                    r, z, w = hold(res_next[l], z_next[l], w_bf[m])
                    out = r + jnp.dot(z, w, preferred_element_type=F32)
                    res_next[l + 1] = out
            elif op == 'H':
                red, mh, wh = hold(red_head, mom_head, w_head)
                nm = momentum * mh + red.astype(F32)
                nw = wh - learn_rate * nm
                box['head'] = (nw, nm)
                out = nm
            token[0] = out

        for op, l, k in ORDER:
            step(op, l, k)
        new_head, new_mom_head = box['head']
        _, logits_next = pool_logits(res_next[layers], images, new_head.astype(jnp.bfloat16))
        return logits_next, new[0][0], new[1][0], new_head, new[0][1], new[1][1], new_mom_head

    batch_spec = P(BATCH_AXES)
    whole_spec = P()
    return jax.shard_map(local_step, mesh=mesh,
                         in_specs=(batch_spec, batch_spec, batch_spec) + (whole_spec,) * 8,
                         out_specs=(batch_spec,) + (whole_spec,) * 6,
                         check_vma=False)
```

```python
import functools

import jax
import jax.numpy as jnp
from jax import lax
from jax.experimental import pallas as pl
from jax.experimental.pallas import tpu as pltpu
from jax.sharding import PartitionSpec as P


LN_EPS = 1e-6
BATCH_AXES = ('rep', 'data')
NB = 8
HB = 512
NS = 4
LINKS = (1, 2, 4)
ADMIT = ((5, 0), (5, 1), (4, 1), (3, 1), (3, 0), (4, 0), (1, 0), (1, 1), (0, 0), (2, 0), (2, 1), (0, 1),)
GATHER_SC = ((0, 0), (0, 1), (3, 1), (4, 0), (5, 1),)
ORDER = tuple((t[0], int(t[1]), int(t[2])) for t in (
    'B50', 'a50', 'a51', 'B40', 'a41', 'B30', 'a31', 'a30', 'a40', 'b50', 'b51', 'B20',
    'b41', 'b31', 'b30', 'b40', 'B10', 'a10', 'c50', 'c31', 'c41', 'c30', 'c51', 'd50',
    'a11', 'c40', 'd41', 'd31', 'B00', 'a00', 'a20', 'b10', 'e50', 'd30', 'a21', 'd51',
    'a01', 'b11', 'H00', 'd40', 'e41', 'U31', 'b00', 'c10', 'b20', 'e30', 'f50', 'U51',
    'c11', 'b21', 'b01', 'f41', 'd10', 'c00', 'U40', 'f30', 'c20', 'c21', 'd00', 'h50',
    'U50', 'h41', 'd11', 'c01', 'h30', 'd21', 'e10', 'U30', 'd20', 'e11', 'd01', 'K00',
    'f10', 'e20', 'e21', 'f11', 'U41', 'f20', 'K01', 'h10', 'f21', 'h11', 'K10', 'h20',
    'K11', 'h21', 'K20', 'K21', 'F30', 'F31', 'F40', 'F41', 'F50', 'F51',
))


def layer_norm(residual):
    centered = residual - jnp.mean(residual, axis=-1, keepdims=True)
    inv_std = lax.rsqrt(jnp.mean(centered * centered, axis=-1, keepdims=True) + LN_EPS)
    return centered * inv_std, inv_std


def norm_back(normed, inv_std, grad_out):
    return inv_std * (grad_out - jnp.mean(grad_out, axis=-1, keepdims=True)
                      - normed * jnp.mean(grad_out * normed, axis=-1, keepdims=True))


def gelu(pre_act):
    return pre_act * (0.5 * (1.0 + lax.erf(pre_act * 0.7071067811865476)))


def gelu_parts(pre_act):
    gauss_cdf = 0.5 * (1.0 + lax.erf(pre_act * 0.7071067811865476))
    density = jnp.exp(-0.5 * pre_act * pre_act) * 0.3989422804014327
    return pre_act * gauss_cdf, gauss_cdf + pre_act * density


def pool_logits(residual, images, head_bf):
    pooled = jnp.mean(residual.reshape(images, -1, residual.shape[-1]), axis=1).astype(jnp.bfloat16)
    return pooled, jnp.dot(pooled, head_bf, preferred_element_type=jnp.float32)


def order_of(m):
    i = ADMIT.index(m) % 3
    return tuple(LINKS[(i + s) % 3] for s in range(3))


def unmask(block, order):
    return ((block // order[0]) % 2) * 4 + ((block // order[1]) % 2) * 2 + (block // order[2]) % 2


def flip(a, b):
    out = 0
    for v in (1, 2, 4):
        x, y = (a // v) % 2, (b // v) % 2
        out = out + (x + y - 2 * x * y) * v
    return out


def place():
    rep, data = lax.axis_index('rep'), lax.axis_index('data')
    return rep, data, rep * 2 + data // 2, data % 2


def dot(a, b, ca=1, cb=0):
    return lax.dot_general(a, b, (((ca,), (cb,)), ((), ())), preferred_element_type=jnp.float32)


def add_bf(a, b):
    return (a.astype(jnp.float32) + b.astype(jnp.float32)).astype(jnp.bfloat16)


ANY = pl.BlockSpec(memory_space=pl.ANY)
WHOLE = pl.BlockSpec(memory_space=pltpu.VMEM)
DMA = pltpu.SemaphoreType.DMA
F32, BF16 = jnp.float32, jnp.bfloat16


def back_body(l, last, order_up, order_down, v_hbm, d_hbm, r_hbm, w1_ref, w2_ref, slope_ref, z_ref, *refs):
    up_s, up_k, down_s, down_k = refs[:4]
    refs = refs[4:]
    if not last:
        dn_hbm, vn_hbm = refs[:2]
        refs = refs[2:]
    (w1, w2, sl, zb, v_ref, d_ref, r_ref, at_own, at_far, v_own, v_far, mine, far, got, acc,
     in_sem, one_sem, out_sem, send_sem, recv_sem) = refs
    rep, data, chip, core = place()
    peer = (rep, data + 1 - 2 * core)
    barrier = pltpu.get_barrier_semaphore()

    def load(i, slot):
        cols = pl.ds(pl.multiple_of(i * HB, HB), HB)
        return (pltpu.make_async_copy(w2_ref.at[l, cols, :], w2.at[slot], in_sem.at[0, slot]),
                pltpu.make_async_copy(slope_ref.at[l, :, cols], sl.at[slot], in_sem.at[1, slot]),
                pltpu.make_async_copy(z_ref.at[l, :, cols], zb.at[slot], in_sem.at[2, slot]),
                pltpu.make_async_copy(w1_ref.at[l, :, cols], w1.at[slot], in_sem.at[3, slot]))

    def start(i, slot):
        for copy in load(i, slot):
            copy.start()

    def remote(i, k):
        return pltpu.make_async_remote_copy(
            src_ref=far.at[i % NS, k], dst_ref=got.at[i % NS, k],
            send_sem=send_sem.at[i % NS, k], recv_sem=recv_sem.at[i % NS, k],
            device_id=peer, device_id_type=pl.DeviceIdType.MESH)

    def stores(i):
        block = flip(i, chip)
        out = []
        for k, (os, ok, order) in enumerate(((up_s, up_k, order_up), (down_s, down_k, order_down))):
            pos = unmask(block, order)
            out.append((pos // 4, pltpu.make_async_copy(mine.at[i % NS, k], os.at[pos % 4], out_sem.at[i % NS, k]),
                        pltpu.make_async_copy(mine.at[i % NS, k], ok.at[pos % 4], out_sem.at[i % NS, k])))
        return out

    def finish(i):
        for k in (0, 1):
            remote(i, k).wait_recv()
            mine[i % NS, k] = add_bf(mine[i % NS, k], got[i % NS, k])
        for high, to_send, to_keep in stores(i):
            @pl.when(high == 1)
            def _():
                to_send.start()

            @pl.when(high == 0)
            def _():
                to_keep.start()

    def settle(i):
        for k in (0, 1):
            remote(i, k).wait_send()
        for high, to_send, to_keep in stores(i):
            @pl.when(high == 1)
            def _():
                to_send.wait()

            @pl.when(high == 0)
            def _():
                to_keep.wait()

    pl.semaphore_signal(barrier, inc=1, device_id=peer, device_id_type=pl.DeviceIdType.MESH)
    get_v = pltpu.make_async_copy(v_hbm, v_ref, one_sem.at[0])
    get_r = pltpu.make_async_copy(r_hbm.at[l], r_ref, one_sem.at[1])
    get_r.start()
    get_v.start()
    start(0, 0)
    start(1, 1)
    if not last:
        get_d = pltpu.make_async_copy(d_hbm, d_ref, one_sem.at[2])
        get_d.start()
    get_r.wait()
    residual = r_ref[...]
    normed, inv_std = layer_norm(residual)
    a_t = normed.astype(BF16).T
    own, other = pl.ds(pl.multiple_of(core * HB, HB), HB), pl.ds(pl.multiple_of((1 - core) * HB, HB), HB)
    acc[...] = jnp.zeros_like(acc)
    at_own[...] = a_t[:HB]
    at_far[...] = a_t[HB:]
    get_v.wait()
    v_own[...] = v_ref[:, own]
    v_far[...] = v_ref[:, other]

    @pl.when(core == 1)
    def _():
        tmp = at_own[...]
        at_own[...] = at_far[...]
        at_far[...] = tmp

    pl.semaphore_wait(barrier, 1)

    def step(i, _):
        slot = i % 3

        @pl.when(i + 2 < NB)
        def _():
            start(i + 2, (i + 2) % 3)

        @pl.when(i >= NS)
        def _():
            settle(i - NS)

        copies = load(i, slot)
        copies[0].wait()
        copies[1].wait()
        s = (dot(v_ref[...], w2[slot].astype(BF16), 1, 1) * sl[slot]).astype(BF16)
        far[i % NS, 0] = dot(at_far[...], s).astype(BF16)
        remote(i, 0).start()
        copies[2].wait()
        z_t = zb[slot].T
        far[i % NS, 1] = dot(z_t, v_far[...]).astype(BF16)
        remote(i, 1).start()
        mine[i % NS, 0] = dot(at_own[...], s).astype(BF16)
        mine[i % NS, 1] = dot(z_t, v_own[...]).astype(BF16)
        copies[3].wait()
        if not last:
            acc[...] += dot(s, w1[slot].astype(BF16), 1, 1)

        @pl.when(i > 0)
        def _():
            finish(i - 1)

        return 0

    lax.fori_loop(0, NB, step, 0)
    if not last:
        get_d.wait()
        residual = r_ref[...]
        normed, inv_std = layer_norm(residual)
        grad = d_ref[...] + norm_back(normed, inv_std, acc[...])
        d_ref[...] = grad
        v_ref[...] = grad.astype(BF16)
        put_d = pltpu.make_async_copy(d_ref, dn_hbm, one_sem.at[2])
        put_v = pltpu.make_async_copy(v_ref, vn_hbm, one_sem.at[0])
        put_d.start()
        put_v.start()
    finish(NB - 1)
    for i in range(NB - NS, NB):
        settle(i)
    if not last:
        put_d.wait()
        put_v.wait()


def back(l, v, d, r, w_up, w_down, slope, z):
    rows, dim, hid = 512, 1024, 4096
    last = l == 0
    tile = jax.ShapeDtypeStruct((4, HB, HB), BF16)
    outs, specs = [tile] * 4, [ANY] * 4
    if not last:
        outs += [jax.ShapeDtypeStruct((rows, dim), F32), jax.ShapeDtypeStruct((rows, dim), BF16)]
        specs += [ANY, ANY]
    return pl.pallas_call(
        functools.partial(back_body, l, last, order_of((l, 0)), order_of((l, 1))),
        out_shape=outs, in_specs=[ANY] * 7, out_specs=specs,
        scratch_shapes=[pltpu.VMEM((3, dim, HB), F32), pltpu.VMEM((3, HB, dim), F32), pltpu.VMEM((3, rows, HB), F32),
                        pltpu.VMEM((3, rows, HB), BF16), pltpu.VMEM((rows, dim), BF16), pltpu.VMEM((rows, dim), F32),
                        pltpu.VMEM((rows, dim), F32), pltpu.VMEM((HB, rows), BF16), pltpu.VMEM((HB, rows), BF16),
                        pltpu.VMEM((rows, HB), BF16), pltpu.VMEM((rows, HB), BF16),
                        pltpu.VMEM((NS, 2, HB, HB), BF16), pltpu.VMEM((NS, 2, HB, HB), BF16),
                        pltpu.VMEM((NS, 2, HB, HB), BF16), pltpu.VMEM((rows, dim), F32),
                        DMA((4, 3)), DMA((3,)), DMA((NS, 2)), DMA((NS, 2)), DMA((NS, 2))],
        compiler_params=pltpu.CompilerParams(collective_id=l, has_side_effects=True, vmem_limit_bytes=60 << 20),
        cost_estimate=pl.CostEstimate(flops=8 * rows * dim * hid, bytes_accessed=60 << 20, transcendentals=0),
        name='back')(v, d, r, w_up, w_down, slope, z)


def add_body(n, a_ref, b_ref, *refs):
    outs, (a, b, in_sem, out_sem) = refs[:-4], refs[-4:]
    order = list(range(n // 2, n)) + list(range(n // 2)) if n > 1 else [0]

    def copies(i):
        return (pltpu.make_async_copy(a_ref.at[i], a.at[i], in_sem.at[0, i]),
                pltpu.make_async_copy(b_ref.at[i], b.at[i], in_sem.at[1, i]))

    done = []
    for i in order:
        for c in copies(i):
            c.start()
    for i in order:
        for c in copies(i):
            c.wait()
        a[i] = add_bf(a[i], b[i])
        if n == 1:
            dst = outs[0].at[0]
        elif i >= n // 2:
            dst = outs[0].at[i - n // 2]
        else:
            dst = outs[1].at[i]
        c = pltpu.make_async_copy(a.at[i], dst, out_sem.at[i])
        c.start()
        done.append(c)
    for c in done:
        c.wait()


def add_halves(a, b):
    n = a.shape[0]
    out = jax.ShapeDtypeStruct((max(n // 2, 1), HB, HB), BF16)
    count = 2 if n > 1 else 1
    return pl.pallas_call(
        functools.partial(add_body, n), out_shape=[out] * count, in_specs=[ANY, ANY], out_specs=[ANY] * count,
        scratch_shapes=[pltpu.VMEM((n, HB, HB), BF16), pltpu.VMEM((n, HB, HB), BF16), DMA((2, n)), DMA((n,))],
        cost_estimate=pl.CostEstimate(flops=n << 29, bytes_accessed=3 * n << 19, transcendentals=0),
        name='add')(a, b)


def cat_body(a_ref, b_ref, o_ref, buf, in_sem, out_sem):
    n = a_ref.shape[0]
    loads = [pltpu.make_async_copy((a_ref if i < n else b_ref).at[i % n], buf.at[i], in_sem.at[i]) for i in range(2 * n)]
    stores = [pltpu.make_async_copy(buf.at[i], o_ref.at[i], out_sem.at[i]) for i in range(2 * n)]
    for c in loads:
        c.start()
    for c, d in zip(loads, stores):
        c.wait()
        d.start()
    for d in stores:
        d.wait()


def cat_halves(a, b):
    n = 2 * a.shape[0]
    return pl.pallas_call(
        cat_body, out_shape=jax.ShapeDtypeStruct((n, HB, HB), BF16), in_specs=[ANY, ANY], out_specs=ANY,
        scratch_shapes=[pltpu.VMEM((n, HB, HB), BF16), DMA((n,)), DMA((n,))],
        cost_estimate=pl.CostEstimate(flops=n << 29, bytes_accessed=2 * n << 19, transcendentals=0),
        name='cat')(a, b)


def fwd_body(layers, x_ref, w1_ref, w2_ref, rs_ref, z_ref, slope_ref, w1, w2, res, keep, act, zs, ss, in_sem, out_sem, res_sem):
    total = layers * NB

    def load(t):
        l, cols = t // NB, pl.ds(pl.multiple_of((t % NB) * HB, HB), HB)
        return (pltpu.make_async_copy(w1_ref.at[l, :, cols], w1.at[t % 4], in_sem.at[0, t % 4]),
                pltpu.make_async_copy(w2_ref.at[l, cols, :], w2.at[t % 4], in_sem.at[1, t % 4]))

    def store(t):
        l, cols = t // NB, pl.ds(pl.multiple_of((t % NB) * HB, HB), HB)
        return (pltpu.make_async_copy(zs.at[t % 3], z_ref.at[l, :, cols], out_sem.at[0, t % 3]),
                pltpu.make_async_copy(ss.at[t % 3], slope_ref.at[l, :, cols], out_sem.at[1, t % 3]))

    def store_res(l):
        return pltpu.make_async_copy(keep.at[l % 2], rs_ref.at[l], res_sem.at[l % 2])

    def prefetch(t):
        @pl.when(t < total)
        def _():
            for c in load(t):
                c.start()

    def first(t):
        @pl.when(t >= 3)
        def _():
            for c in store(t - 3):
                c.wait()

        hidden, slope = gelu_parts(dot(act[...], w1[t % 4].astype(BF16)))
        zs[t % 3] = hidden.astype(BF16)
        ss[t % 3] = slope
        for c in store(t):
            c.start()

    def second(t):
        res[...] += dot(zs[t % 3], w2[t % 4].astype(BF16))

    for t in (0, 1, 2):
        for c in load(t):
            c.start()
    res[...] = x_ref[...].astype(F32)

    def block(l, _):
        t0 = l * NB

        @pl.when(l >= 2)
        def _():
            store_res(l - 2).wait()

        residual = res[...]
        keep[l % 2] = residual
        store_res(l).start()
        act[...] = layer_norm(residual)[0].astype(BF16)
        load(t0)[0].wait()
        first(t0)

        def step(i, _):
            t = t0 + i
            prefetch(t + 2)
            load(t)[0].wait()
            load(t - 1)[1].wait()

            @pl.when(t >= 3)
            def _():
                for c in store(t - 3):
                    c.wait()

            res[...] += dot(zs[(t - 1) % 3], w2[(t - 1) % 4].astype(BF16))
            hidden, slope = gelu_parts(dot(act[...], w1[t % 4].astype(BF16)))
            zs[t % 3] = hidden.astype(BF16)
            ss[t % 3] = slope
            for c in store(t):
                c.start()
            return 0

        lax.fori_loop(1, NB, step, 0)
        load(t0 + NB - 1)[1].wait()
        second(t0 + NB - 1)
        prefetch(t0 + NB + 2)
        return 0

    lax.fori_loop(0, layers, block, 0)

    store_res(layers - 2).wait()
    keep[layers % 2] = res[...]
    store_res(layers).start()
    for t in range(total - 3, total):
        for c in store(t):
            c.wait()
    for l in (layers - 1, layers):
        store_res(l).wait()


def forward(x, w_up, w_down):
    rows, dim, hid, layers = 512, 1024, 4096, 6
    return pl.pallas_call(
        functools.partial(fwd_body, layers),
        out_shape=[jax.ShapeDtypeStruct((layers + 1, rows, dim), F32), jax.ShapeDtypeStruct((layers, rows, hid), BF16),
                   jax.ShapeDtypeStruct((layers, rows, hid), F32)],
        in_specs=[WHOLE, ANY, ANY], out_specs=[ANY, ANY, ANY],
        scratch_shapes=[pltpu.VMEM((4, dim, HB), F32), pltpu.VMEM((4, HB, dim), F32), pltpu.VMEM((rows, dim), F32),
                        pltpu.VMEM((2, rows, dim), F32), pltpu.VMEM((rows, dim), BF16), pltpu.VMEM((3, rows, HB), BF16),
                        pltpu.VMEM((3, rows, HB), F32), DMA((2, 4)), DMA((2, 3)), DMA((2,))],
        compiler_params=pltpu.CompilerParams(vmem_limit_bytes=50 << 20),
        cost_estimate=pl.CostEstimate(flops=24 * rows * dim * hid, bytes_accessed=280 << 20, transcendentals=0),
        name='forward')(x, w_up, w_down)


def update_body(l, k, kind, order, sc, into, rates_ref, *refs):
    acts = ()
    if kind == 'up':
        acts, refs = refs[:1], refs[1:]
    elif kind == 'down':
        acts, refs = refs[:2], refs[2:]
    pieces = 1 if sc else 4
    grads, refs = refs[:pieces], refs[pieces:]
    w_ref, m_ref = refs[:2]
    refs = refs[4:] if into else refs[2:]
    nw_ref, nm_ref, out_ref = refs[:3]
    w, m, g, ob, act, in_sem, act_sem, out_sem, ob_sem = refs[3:]
    _, _, chip, core = place()
    lr, mu = rates_ref[0], rates_ref[1]
    sides = [pl.ds(pl.multiple_of(core * HB, HB), HB), pl.ds(pl.multiple_of((1 - core) * HB, HB), HB)]
    slots = 6

    def natural(i):
        cube = 0
        for s, v in enumerate(order):
            cube = cube + ((i // (4 >> s)) % 2) * v
        return flip(cube, chip)

    def span(i):
        return pl.ds(pl.multiple_of(natural(i) * HB, HB), HB)

    def at(i, h):
        return (l, sides[h], span(i)) if k == 0 else (l, span(i), sides[h])

    def load(i, h):
        slot = (2 * i + h) % slots
        return (pltpu.make_async_copy(w_ref.at[at(i, h)], w.at[slot], in_sem.at[0, slot]),
                pltpu.make_async_copy(m_ref.at[at(i, h)], m.at[slot], in_sem.at[1, slot]))

    def load_act(i):
        return pltpu.make_async_copy(acts[1].at[:, span(i)], act.at[i % 3], act_sem.at[i % 3])

    def load_grad(i, h, high):
        slot = (2 * i + h) % slots
        src = grads[0].at[natural(i) * 2 + (core if h == 0 else 1 - core)] if sc else grads[2 * h + high].at[i % 4]
        return pltpu.make_async_copy(src, g.at[slot], in_sem.at[2, slot])

    def start(i, h):
        for c in load(i, h):
            c.start()
        if kind == 'down' and h == 0:
            load_act(i).start()
        if sc:
            load_grad(i, h, 0).start()
            return
        for high in (0, 1):
            @pl.when(i // 4 == high)
            def _():
                load_grad(i, h, high).start()

    def store(i, h):
        slot = (2 * i + h) % slots
        return (pltpu.make_async_copy(w.at[slot], nw_ref.at[at(i, h)], out_sem.at[0, slot]),
                pltpu.make_async_copy(m.at[slot], nm_ref.at[at(i, h)], out_sem.at[1, slot]))

    def store_last(i, h):
        if kind == 'up':
            return pltpu.make_async_copy(ob.at[i % 2], out_ref.at[:, span(i)], ob_sem.at[i % 2])
        return pltpu.make_async_copy(ob.at[i % 2, h], out_ref.at[at(i, h)[1:]], ob_sem.at[i % 2, h])

    def whole_last(i):
        return (store_last(i, 0),) if kind == 'up' else (store_last(i, 0), store_last(i, 1))

    start(0, 0)
    start(0, 1)
    start(1, 0)
    if kind == 'up':
        residual = acts[0][...]
        normed = layer_norm(residual)[0].astype(BF16)
        act[...] = normed
    elif kind == 'down':
        out_ref[...] = acts[0][...]

    def step(i, _):
        pre = None
        if kind != 'down':
            @pl.when(i >= 2)
            def _():
                for c in whole_last(i - 2):
                    c.wait()
        for h in (0, 1):
            slot = (2 * i + h) % slots
            ahead, side = (i + 1, 1) if h == 0 else (i + 2, 0)
            back_i, back_h = (i - 2, 1) if h == 0 else (i - 1, 0)

            @pl.when(ahead < NB)
            def _():
                @pl.when(back_i >= 0)
                def _():
                    for c in store(back_i, back_h):
                        c.wait()

                start(ahead, side)

            for c in load(i, h):
                c.wait()
            load_grad(i, h, 0).wait()
            new_m = mu * m[slot] + g[slot].astype(F32)
            new_w = w[slot] - lr * new_m
            m[slot] = new_m
            w[slot] = new_w
            for c in store(i, h):
                c.start()
            new_bf = new_w.astype(BF16)
            if kind == 'up':
                part = dot(act[:, sides[h]], new_bf)
                pre = part if h == 0 else pre + part
            elif kind == 'down':
                if h == 0:
                    load_act(i).wait()
                out_ref[:, sides[h]] += dot(act[i % 3], new_bf)
            else:
                ob[i % 2, h] = new_bf
        if kind == 'up':
            ob[i % 2] = gelu(pre).astype(BF16)
        if kind != 'down':
            for c in whole_last(i):
                c.start()
        return 0

    lax.fori_loop(0, NB, step, 0)
    for s in range(2 * NB - 6, 2 * NB):
        for c in store(s // 2, s % 2):
            c.wait()
    if kind != 'down':
        for i in range(NB - 2, NB):
            for c in whole_last(i):
                c.wait()


def update(m, kind, rates, acts, grads, w, mom, into):
    l, k = m
    dim, hid, rows = 1024, 4096, 512
    sc = len(grads) == 1
    ob_sem = DMA((2,))
    if kind == 'up':
        act_specs, last, last_spec = [WHOLE], jax.ShapeDtypeStruct((rows, hid), BF16), ANY
        ob, act = (2, rows, HB), (rows, dim)
    elif kind == 'down':
        act_specs, last, last_spec = [WHOLE, ANY], jax.ShapeDtypeStruct((rows, dim), F32), WHOLE
        ob, act = (2, 16, 128), (3, rows, HB)
    else:
        act_specs, last_spec = [], ANY
        last = jax.ShapeDtypeStruct((dim, hid) if k == 0 else (hid, dim), BF16)
        ob, act = (2, 2, HB, HB), (16, 128)
        ob_sem = DMA((2, 2))
    in_specs = [pl.BlockSpec(memory_space=pltpu.SMEM)] + act_specs + [ANY] * (len(grads) + 2)
    args = [rates, *acts, *grads, w, mom]
    aliases = {}
    if into is not None:
        aliases = {len(args): 0, len(args) + 1: 1}
        in_specs += [ANY, ANY]
        args += list(into)
    full = jax.ShapeDtypeStruct(w.shape, F32)
    return pl.pallas_call(
        functools.partial(update_body, l, k, kind, order_of(m), sc, into is not None),
        out_shape=[full, full, last], in_specs=in_specs, out_specs=[ANY, ANY, last_spec],
        scratch_shapes=[pltpu.VMEM((6, HB, HB), F32), pltpu.VMEM((6, HB, HB), F32), pltpu.VMEM((6, HB, HB), BF16),
                        pltpu.VMEM(ob, BF16), pltpu.VMEM(act, BF16),
                        DMA((3, 6)), DMA((3,)), DMA((2, 6)), ob_sem],
        input_output_aliases=aliases,
        compiler_params=pltpu.CompilerParams(vmem_limit_bytes=48 << 20),
        cost_estimate=pl.CostEstimate(flops=10_000_000_000, bytes_accessed=80 << 20, transcendentals=0))(*args)


def solution(mesh):
    num_dev = mesh.shape['rep'] * mesh.shape['data']
    pairs = {v: [(i, i ^ max(2 * v, 1)) for i in range(num_dev)] for v in (0, 1, 2, 4)}

    def local_step(x_now, x_next, labels, w_up, w_down, w_head, mom_up, mom_down, mom_head, learn_rate, momentum):
        images, seq_len, model_dim = x_now.shape
        layers = w_up.shape[0]
        classes = w_head.shape[1]
        rows = images * seq_len
        global_batch = images * num_dev
        weights = (w_up, w_down)
        moms = (mom_up, mom_down)
        rates = jnp.stack([learn_rate, momentum])
        token = [None]

        def hold(*args):
            if token[0] is None:
                return args
            return lax.optimization_barrier((*args, token[0]))[:-1]

        def cp(x, link):
            return lax.ppermute(x, BATCH_AXES, pairs[link])

        stream, hidden, slopes = forward(x_now.reshape(rows, model_dim), w_up, w_down)
        residual = stream[layers]
        head_bf = w_head.astype(BF16)
        pooled, logits = pool_logits(residual, images, head_bf)
        soft_probs = jax.nn.softmax(logits, axis=-1)
        onehot = (labels[:, None] == jnp.arange(classes, dtype=jnp.int32)[None, :]).astype(F32)
        d_logits = ((soft_probs - onehot) / global_batch).astype(BF16)
        grad_head = jnp.einsum('bd,bc->dc', pooled, d_logits, preferred_element_type=F32)
        red_head = lax.psum(grad_head.astype(BF16), BATCH_AXES)
        d_pooled = jnp.einsum('bc,dc->bd', d_logits, head_bf, preferred_element_type=F32)
        d_resid = jnp.broadcast_to((d_pooled / seq_len)[:, None, :], (images, seq_len, model_dim)).reshape(rows, model_dim)

        d_res, v_bf = d_resid, d_resid.astype(BF16)
        box = {}
        new = [None, None]
        res_next = {0: x_next.reshape(rows, model_dim).astype(F32)}
        z_next = {}
        w_bf = {}

        def step(op, l, k):
            nonlocal d_res, v_bf
            m = (l, k)
            order = order_of(m)
            if op == 'B':
                v, d = hold(v_bf, d_res)
                out = back(l, v, d, stream, w_up, w_down, slopes, hidden)
                for j in (1, 0):
                    box['s1', (l, j)], box['k1', (l, j)] = out[2 * j], out[2 * j + 1]
                if l > 0:
                    d_res, v_bf = out[4:]
                out = out[3]
            elif op == 'a':
                send, = hold(box.pop(('s1', m)))
                box['r1', m] = cp(send, order[0])
                return
            elif op in 'bc':
                src, dst = {'b': ('1', '2'), 'c': ('2', '3')}[op]
                keep, got = hold(box.pop(('k' + src, m)), box.pop(('r' + src, m)))
                out, box['k' + dst, m] = add_halves(keep, got)
                box['r' + dst, m] = cp(out, order[1] if op == 'b' else order[2])
                out = box['k' + dst, m]
            elif op == 'd':
                keep, got = hold(box.pop(('k3', m)), box.pop(('r3', m)))
                out, = add_halves(keep, got)
                if m in GATHER_SC:
                    box['g', m] = (lax.all_gather(out, BATCH_AXES).reshape(num_dev, HB, HB),)
                else:
                    box['p0', m] = out
                    box['q0', m] = cp(out, order[2])
            elif op in 'ef':
                src, dst = {'e': ('0', '1'), 'f': ('1', '2')}[op]
                own, got = hold(box.pop(('p' + src, m)), box.pop(('q' + src, m)))
                out = cat_halves(own, got)
                if op == 'e':
                    box['p1', m] = out
                    box['q1', m] = cp(out, order[1])
                else:
                    far = cp(out, order[0])
                    box['g', m] = (out, far, cp(out, 0))
            elif op == 'h':
                own, far, other = box['g', m]
                send, = hold(far)
                box['g', m] = (own, far, other, cp(send, 0))
                return
            elif op in 'KU':
                kind = 'plain' if op == 'U' else ('up' if k == 0 else 'down')
                acts = ()
                if kind == 'up':
                    acts = (res_next[l],)
                elif kind == 'down':
                    acts = (res_next[l], z_next[l])
                held = hold(*acts, *box.pop(('g', m)))
                acts, grads = held[:len(acts)], held[len(acts):]
                nw, nm, out = update(m, kind, rates, acts, grads, weights[k], moms[k], new[k])
                new[k] = (nw, nm)
                if kind == 'up':
                    z_next[l] = out
                elif kind == 'down':
                    res_next[l + 1] = out
                else:
                    w_bf[m] = out
            elif op == 'F':
                if k == 0:
                    r, w = hold(res_next[l], w_bf[m])
                    out = gelu(jnp.dot(layer_norm(r)[0].astype(BF16), w, preferred_element_type=F32)).astype(BF16)
                    z_next[l] = out
                else:
                    r, z, w = hold(res_next[l], z_next[l], w_bf[m])
                    out = r + jnp.dot(z, w, preferred_element_type=F32)
                    res_next[l + 1] = out
            elif op == 'H':
                red, mh, wh = hold(red_head, mom_head, w_head)
                nm = momentum * mh + red.astype(F32)
                nw = wh - learn_rate * nm
                box['head'] = (nw, nm)
                out = nm
            token[0] = out

        for op, l, k in ORDER:
            step(op, l, k)
        new_head, new_mom_head = box['head']
        _, logits_next = pool_logits(res_next[layers], images, new_head.astype(jnp.bfloat16))
        return logits_next, new[0][0], new[1][0], new_head, new[0][1], new[1][1], new_mom_head

    batch_spec = P(BATCH_AXES)
    whole_spec = P()
    return jax.shard_map(local_step, mesh=mesh,
                         in_specs=(batch_spec, batch_spec, batch_spec) + (whole_spec,) * 8,
                         out_specs=(batch_spec,) + (whole_spec,) * 6,
                         check_vma=False)
```
